256 devices in a mesh: feat: 64 (over y, x, z_lo), rep: 4 (over z_hi, core).
Axes of the slice: x: 4, y: 4, z: 8 (z_hi: 2, z_lo: 4; z = z_hi * 4 + z_lo), core: 2. Of those that a mesh axis runs over, the one named last changes fastest.
Arguments:
- features: bfloat16 [4, 64, 1024, 512], P('rep', None, 'feat'), may hold values from -6 to 6
- adjacency_one: int32 [4, 64, 5, 16, 512], P('rep'), may hold values from 0 to 65535, as said below
- pre_hidden: bfloat16 [4, 64, 256, 256], P('rep', 'feat'), may hold values from -6 to 6
- adjacency_two: int32 [4, 64, 5, 8, 256], P('rep', 'feat'), may hold values from 0 to 65535, as said below
- weight_two: bfloat16 [6, 256, 256], replicated, may hold values from -0.375 to 0.375
- out_grad: bfloat16 [4, 64, 128, 256], P('rep', 'feat'), may hold values from -6 to 6
Outputs:
- grad_w1: float32 [6, 1024, 256], P(None, 'feat')
- grad_b1: float32 [256], replicated
- grad_w2: float32 [6, 256, 256], replicated
- grad_b2: float32 [256], replicated
The draws below stay inside these ranges and needn't reach their ends.
Inputs may be any that keep to these rules, and one draw needn't show every extreme that they name: `adjacency_one`: bit k, k below 16, of word (w, n) is the entry of destination row 16 w + k and source column n; higher bits are zero; some rows are empty. `adjacency_two`: bit k, k below 16, of word (w, n) is the entry of seed row 16 w + k and source column n; higher bits are zero; some rows are empty.
All inputs are finite; a program needn't handle non-finite values.
Results may differ from the reference program's by a relative error of at most 0.0041.
Values may be sent and summed in bfloat16 or wider, within the bound.
A program may use at most 128 MiB of HBM per device.

```python
import jax
import jax.numpy as jnp
from jax import lax

F = 1024
H = 256
R = 5
SEEDS = 128
DST1 = 256
NB = 512
GROUPS = 4
BATCHES = 64


def packed_bits(key, leading, row_count, col_count):
    density_key, ticket_key = jax.random.split(key)
    density = jax.random.randint(density_key, leading + (row_count, 1), 0, 5)
    ticket = jax.random.randint(ticket_key, leading + (row_count, col_count), 0, 16)
    entries = (ticket < 3 * density).astype(jnp.int32)
    grouped = entries.reshape(leading + (row_count // 16, 16, col_count))
    shifts = jnp.arange(16, dtype=jnp.int32)
    return jnp.sum(jnp.left_shift(grouped, shifts[:, None]), axis=-2).astype(jnp.int32)


def draw_adjacency_one(key, part):
    return packed_bits(jax.random.fold_in(key, 11), (GROUPS, BATCHES, R), DST1, NB)


def draw_adjacency_two(key, part):
    return packed_bits(jax.random.fold_in(key, 12), (GROUPS, BATCHES, R), SEEDS, DST1)


def shard_levels(own_key, dims, cuts, smallest, high):
    gain, own = 1.0, jax.random.fold_in(own_key, 6)
    for position, shards_of in cuts:
        heights = jnp.exp(jax.random.uniform(jax.random.fold_in(own, position), (shards_of,), jnp.float32, smallest / len(cuts), high / len(cuts)))
        gain = gain * jnp.repeat(heights, dims[position] // shards_of).reshape([-1 if axis == position else 1 for axis in range(len(dims))])
    return gain


def centred(rng, extent, scale, limit, cuts=(), held_as=jnp.bfloat16):
    drawn = scale * jax.random.normal(rng, extent, jnp.float32)
    if cuts:
        drawn = drawn * shard_levels(rng, extent, cuts, -0.22, 0.18)
    return jnp.clip(drawn, -limit, limit).astype(held_as)


def setup_inputs(seed: int = 0) -> dict:
    key_of = jax.random.split(jax.random.key(seed), 7)
    features = centred(key_of[0], (GROUPS, BATCHES, F, NB), 1.0, 6.0, ((0, 4), (2, 64)))
    adjacency_one = draw_adjacency_one(jax.random.fold_in(key_of[6], 71), 0)
    pre_hidden = centred(key_of[2], (GROUPS, BATCHES, DST1, H), 1.0, 6.0, ((0, 4), (1, 64)))
    adjacency_two = draw_adjacency_two(jax.random.fold_in(key_of[6], 71), 0)
    weight_two = centred(key_of[4], (R + 1, H, H), H ** -0.5, 0.375)
    out_grad = centred(key_of[5], (GROUPS, BATCHES, SEEDS, H), 1.0, 6.0, ((0, 4), (1, 64)))
    return dict(features=features, adjacency_one=adjacency_one, pre_hidden=pre_hidden, adjacency_two=adjacency_two, weight_two=weight_two, out_grad=out_grad)


def unpack(packed):
    shifts = jnp.arange(16, dtype=jnp.int32)
    spread = jnp.bitwise_and(jnp.right_shift(packed[..., None, :], shifts[:, None]), 1)
    dense = spread.reshape(packed.shape[:-2] + (packed.shape[-2] * 16, packed.shape[-1]))
    degree = jnp.sum(dense, axis=-1).astype(jnp.float32)
    return dense.astype(jnp.float32), 1.0 / jnp.maximum(degree, 1.0)


def reference(features, adjacency_one, pre_hidden, adjacency_two, weight_two, out_grad):
    total_batches = GROUPS * BATCHES
    factor = float(SEEDS * total_batches) ** -0.5
    feat_all = features.reshape((total_batches, F, NB))
    adj_one = adjacency_one.reshape((total_batches,) + adjacency_one.shape[2:])
    pre_all = pre_hidden.reshape((total_batches, DST1, H))
    adj_two = adjacency_two.reshape((total_batches,) + adjacency_two.shape[2:])
    grad_all = out_grad.reshape((total_batches, SEEDS, H))
    weights = weight_two.astype(jnp.float32)

    def one_batch(carry, inputs):
        panel_sum, upper_sum, bias_one, bias_two = carry
        columns, words_one, pre_rows, words_two, grad_rows = inputs
        hidden = jnp.maximum(pre_rows, 0).astype(jnp.float32)
        matrix_two, inverse_two = unpack(words_two)
        mixed = (jnp.einsum('rsd,dh->rsh', matrix_two, hidden) * inverse_two[..., None]).astype(jnp.bfloat16).astype(jnp.float32)
        scaled = grad_rows.astype(jnp.float32) * factor
        scaled_low = scaled.astype(jnp.bfloat16).astype(jnp.float32)
        grad_rel = jnp.einsum('rsh,sk->rhk', mixed, scaled_low)
        grad_self = jnp.einsum('sh,sk->hk', hidden[:SEEDS], scaled_low)
        upper_sum = upper_sum + jnp.concatenate([grad_self[None], grad_rel], 0)
        bias_two = bias_two + jnp.sum(scaled, 0)
        backed = (jnp.einsum('sk,rhk->rsh', scaled_low, weights[1:]) * inverse_two[..., None]).astype(jnp.bfloat16).astype(jnp.float32)
        spread_back = jnp.einsum('rsd,rsh->dh', matrix_two, backed)
        own_part = jnp.einsum('sk,hk->sh', scaled_low, weights[0])
        hidden_total = spread_back + jnp.pad(own_part, ((0, DST1 - SEEDS), (0, 0)))
        hidden_grad = jnp.where(pre_rows > 0, hidden_total, 0.0).astype(jnp.bfloat16).astype(jnp.float32)
        bias_one = bias_one + jnp.sum(hidden_grad, 0)
        matrix_one, inverse_one = unpack(words_one)
        column_f = columns.astype(jnp.float32)
        gathered = (jnp.einsum('rdn,fn->rdf', matrix_one, column_f) * inverse_one[..., None]).astype(jnp.bfloat16).astype(jnp.float32)
        panel_rel = jnp.einsum('rdf,dh->rfh', gathered, hidden_grad)
        panel_self = jnp.einsum('fd,dh->fh', column_f[:, :DST1], hidden_grad)
        panel_sum = panel_sum + jnp.concatenate([panel_self[None], panel_rel], 0)
        return (panel_sum, upper_sum, bias_one, bias_two), None

    start = (jnp.zeros((R + 1, F, H), jnp.float32), jnp.zeros((R + 1, H, H), jnp.float32),
             jnp.zeros((H,), jnp.float32), jnp.zeros((H,), jnp.float32))
    finals, unused = lax.scan(one_batch, start, (feat_all, adj_one, pre_all, adj_two, grad_all))
    return finals[0], finals[2], finals[1], finals[3]
```

```python
import functools

import jax
import jax.numpy as jnp
from jax import lax
from jax.experimental import pallas as pl
from jax.experimental.pallas import tpu as pltpu
from jax.sharding import Mesh
from jax.sharding import PartitionSpec as P

MESH = pl.DeviceIdType.MESH
AXES = ("y", "x", "z", "g", "c")
FEAT = ("y", "x", "z")
REP = ("g", "c")
BF16 = jnp.bfloat16
F32 = jnp.float32
NN = (((1,), (0,)), ((), ()))
NT = (((1,), (1,)), ((), ()))
TN = (((0,), (0,)), ((), ()))


def mm(a, b, dims):
    return lax.dot_general(a, b, dims, preferred_element_type=F32)


def local(src, dst, sem):
    return pltpu.make_async_copy(src, dst, sem)


def spread_bits(words, r, out, rows, width):
    shift = lax.broadcasted_iota(jnp.int32, (16, width), 0)
    for w in range(rows // 16):
        word = jnp.broadcast_to(words[r, pl.ds(w, 1), :], (16, width))
        bits = lax.bitwise_and(lax.shift_right_logical(word, shift), 1)
        out[r, pl.ds(16 * w, 16), :] = bits.astype(F32).astype(BF16)


def kernel(
    dims,
    factor,
    feat,
    adj1,
    pre_any,
    adj2,
    w2_any,
    og_any,
    out1,
    out2,
    outb,
    pre,
    words2,
    w2,
    og,
    words1,
    dense2,
    dense1,
    c1,
    rx,
    hgbuf,
    total,
    acc,
    wg,
    cxs2,
    cxr2,
    s2,
    r2,
    zbuf,
    agbuf,
    agp,
    cxs1,
    cxr1,
    s1,
    r1,
    zhs,
    zhr,
    d1s,
    d1r,
    loc_sem,
    own_sem,
    xs_sem,
    xr_sem,
    hs_sem,
    hr_sem,
    px_sem,
):
    Y, X, Z, G, C = dims
    NP, ZZ = Y * X, Z * G
    y, x, z, g, c = (lax.axis_index(a) for a in AXES)
    me = y * X + x
    zabs = g * Z + z
    relations = words1.shape[0] // Z
    half = (relations + 1) // C
    cw = feat.shape[2]
    h = w2.shape[1]
    hc = h // NP
    seeds = og.shape[0]

    def plane(k, sign):
        yy = lax.rem(y + sign * lax.div(k, X) + Y, Y)
        xx = lax.rem(x + sign * lax.rem(k, X) + X, X)
        return yy * X + xx, (yy, xx, z, g, c)

    def column(zz):
        return (y, x, lax.rem(zz, Z), lax.div(zz, Z), c)

    partner = (y, x, z, g, 1 - c)
    across = (y, x, z, 1 - g, c)

    def remote(src, dst, send, recv, device):
        return pltpu.make_async_remote_copy(
            src_ref=src, dst_ref=dst, send_sem=send, recv_sem=recv, device_id=device, device_id_type=MESH
        )

    barrier = pltpu.get_barrier_semaphore()

    def greet_plane(k, carry):
        pl.semaphore_signal(barrier, inc=1, device_id=plane(k, 1)[1], device_id_type=MESH)
        return carry

    def greet_column(k, carry):
        pl.semaphore_signal(barrier, inc=1, device_id=column(lax.rem(zabs + k, ZZ)), device_id_type=MESH)
        return carry

    lax.fori_loop(1, NP, greet_plane, 0)
    lax.fori_loop(1, ZZ, greet_column, 0)
    pl.semaphore_signal(barrier, inc=1, device_id=partner, device_id_type=MESH)

    base = me * Z
    loads = [
        local(adj2.at[0, 0], words2, loc_sem.at[0]),
        local(pre_any.at[0, 0], pre, loc_sem.at[1]),
        local(og_any.at[0, 0], og, loc_sem.at[2]),
        local(w2_any, w2, loc_sem.at[3]),
    ]
    for q in range(Z):
        loads.append(
            local(adj1.at[0, base + q], words1.at[pl.ds(q * relations, relations)], loc_sem.at[4 + q])
        )
    for load in loads:
        load.start()

    loads[0].wait()
    for r in range(relations):
        spread_bits(words2, r, dense2, seeds, h)
    pl.semaphore_wait(barrier, NP + ZZ - 1)

    for i in range(Z):
        m = lax.rem(z + i, Z)
        local(feat.at[0, base + m], rx.at[m, pl.ds(0, cw), :], own_sem.at[i]).start()

        def send_features(k, carry):
            other, device = plane(k, 1)
            remote(
                feat.at[0, other * Z + m],
                rx.at[m, pl.ds(pl.multiple_of(k * cw, cw), cw), :],
                xs_sem.at[i],
                xr_sem.at[i],
                device,
            ).start()
            return carry

        lax.fori_loop(1, NP, send_features, 0)

    for load in loads[1:4]:
        load.wait()
    hidden = jnp.maximum(pre[...], 0)
    scaled = og[...].astype(F32) * factor
    low = scaled.astype(BF16)
    ones = jnp.ones((h, h), BF16)
    wg[0] = mm(hidden[:seeds], low, TN)
    total[...] = jnp.zeros_like(total)
    total[pl.ds(0, seeds), :] = mm(low, w2[0], NT)
    for r in range(relations):
        dense = dense2[r]
        inverse = 1.0 / jnp.maximum(mm(dense, ones, NN), 1.0)
        mixed = (mm(dense, hidden, NN) * inverse).astype(BF16)
        wg[r + 1] = mm(mixed, low, TN)
        backed = (mm(low, w2[r + 1], NT) * inverse).astype(BF16)
        total[...] += mm(dense, backed, TN)
    grad = jnp.where(pre[...] > 0, total[...], 0.0).astype(BF16)
    hgbuf[z] = grad
    row = lax.broadcasted_iota(jnp.int32, (8, h), 0)
    bias_one = jnp.sum(grad.astype(F32), axis=0, keepdims=True)
    bias_two = jnp.sum(scaled, axis=0, keepdims=True)
    first = c == 0
    bias_keep = jnp.where(row == 0, jnp.where(first, bias_one, bias_two), 0.0)
    bias_give = jnp.where(row == 0, jnp.where(first, bias_two, bias_one), 0.0)
    for q in range(half):
        cxs2[pl.ds(q * h, h), :] = wg[(1 - c) * half + q].astype(BF16)
    cxs2[pl.ds(half * h, 8), :] = bias_give.astype(BF16)
    swap2 = remote(cxs2, cxr2, px_sem.at[0], px_sem.at[1], partner)
    swap2.start()

    def give_grad(k):
        other = lax.rem(z + Z - k, Z)
        return remote(
            hgbuf.at[z], hgbuf.at[z], hs_sem.at[k], hr_sem.at[k], (y, x, other, g, c)
        )

    for k in range(1, Z):
        give_grad(k).start()

    for load in loads[4:]:
        load.wait()
    ones_row = jnp.ones((16, words1.shape[2]), BF16)

    def spread_one(t, carry):
        spread_bits(words1, t, dense1, 16 * words1.shape[1], words1.shape[2])
        count = mm(ones_row, dense1[t], NT)
        c1[t] = 1.0 / jnp.maximum(count[:8], 1.0)
        return carry

    lax.fori_loop(0, Z * relations, spread_one, 0)

    swap2.wait_recv()
    for q in range(half):
        both = wg[c * half + q] + cxr2[pl.ds(q * h, h), :].astype(F32)
        s2[:, pl.ds(q * hc, hc), :] = both.astype(BF16).reshape(NP, hc, h)
    bias = (bias_keep + cxr2[pl.ds(half * h, 8), :].astype(F32)).astype(BF16)
    s2[:, pl.ds(half * hc, 8), :] = jnp.broadcast_to(bias[None], (NP, 8, h))

    def send_second(k, carry):
        other, device = plane(k, 1)
        remote(s2.at[other], r2.at[k], px_sem.at[2], px_sem.at[3], device).start()
        return carry

    lax.fori_loop(1, NP, send_second, 0)

    acc[...] = jnp.zeros_like(acc)
    for i in range(Z):
        m = lax.rem(z + i, Z)
        if i:
            give_grad(i).wait_recv()
        local(feat.at[0, base + m], rx.at[m, pl.ds(0, cw), :], own_sem.at[i]).wait()
        arrived = rx.at[m, pl.ds(cw, (NP - 1) * cw), :]
        local(arrived, arrived, xr_sem.at[i]).wait()
        columns = rx[m]
        grad_m = hgbuf[m]
        acc[0] += mm(columns[:, : grad_m.shape[0]], grad_m, NN)

        def one_relation(r, carry):
            t = m * relations + r
            gathered = (mm(columns, dense1[t], NT) * c1[t][:1]).astype(BF16)
            acc[r + 1] += mm(gathered, grad_m, NN)
            return carry

        lax.fori_loop(0, relations, one_relation, 0)

    for q in range(half):
        cxs1[q] = acc[(1 - c) * half + q].astype(BF16)
    swap1 = remote(cxs1, cxr1, px_sem.at[4], px_sem.at[5], partner)
    swap1.start()

    second_in = r2.at[pl.ds(1, NP - 1)]
    local(second_in, second_in, px_sem.at[3]).wait()
    summed = s2[me].astype(F32)
    for k in range(1, NP):
        summed += r2[k].astype(F32)
    zbuf[zabs] = summed.astype(BF16)

    def send_column(k, carry):
        remote(
            zbuf.at[zabs], zbuf.at[zabs], px_sem.at[6], px_sem.at[7], column(lax.rem(zabs + k, ZZ))
        ).start()
        return carry

    lax.fori_loop(1, ZZ, send_column, 0)

    swap1.wait_recv()
    for q in range(half):
        both = acc[c * half + q] + cxr1[q].astype(F32)
        s1[:, pl.ds(q * cw, cw), :] = both.astype(BF16).reshape(NP, cw, h)

    def send_first(k, carry):
        other, device = plane(k, -1)
        remote(s1.at[k], r1.at[k], px_sem.at[8], px_sem.at[9], device).start()
        return carry

    lax.fori_loop(1, NP, send_first, 0)

    column_in = zbuf.at[pl.ds(0, ZZ - 1)]
    local(column_in, column_in, px_sem.at[7]).wait()
    summed = zbuf[0].astype(F32)
    for k in range(1, ZZ):
        summed += zbuf[k].astype(F32)
    agbuf[me] = summed.astype(BF16)

    def send_everyone(k, carry):
        other, device = plane(k, 1)
        remote(agbuf.at[me], agbuf.at[me], px_sem.at[10], px_sem.at[11], device).start()
        return carry

    lax.fori_loop(1, NP, send_everyone, 0)

    first_in = r1.at[pl.ds(1, NP - 1)]
    local(first_in, first_in, px_sem.at[9]).wait()
    summed = s1[0].astype(F32)
    for k in range(1, NP):
        summed += r1[k].astype(F32)
    zhs[...] = summed.astype(BF16)
    cross = remote(zhs, zhr, px_sem.at[12], px_sem.at[13], across)
    cross.start()

    everyone_in = agbuf.at[pl.ds(0, NP - 1)]
    local(everyone_in, everyone_in, px_sem.at[11]).wait()
    swap3 = remote(agbuf, agp, px_sem.at[14], px_sem.at[15], partner)
    swap3.start()
    for q in range(half):
        out2[c * half + q] = agbuf[:, pl.ds(q * hc, hc), :].astype(F32).reshape(h, h)

    cross.wait_recv()
    final = (zhs[...].astype(F32) + zhr[...].astype(F32)).reshape(half, cw, h)
    d1s[...] = final
    swap4 = remote(d1s, d1r, px_sem.at[16], px_sem.at[17], partner)
    swap4.start()
    out1[pl.ds(c * half, half)] = final

    swap3.wait_recv()
    for q in range(half):
        out2[(1 - c) * half + q] = agp[:, pl.ds(q * hc, hc), :].astype(F32).reshape(h, h)
    kept = agbuf[0, pl.ds(half * hc, 8), :].astype(F32)[:1]
    given = agp[0, pl.ds(half * hc, 8), :].astype(F32)[:1]
    outb[...] = jnp.where(row == c, kept, given)
    swap4.wait_recv()
    out1[pl.ds((1 - c) * half, half)] = d1r[...]

    for i in range(Z):
        sent = feat.at[0, pl.ds(0, NP - 1)]
        local(sent, sent, xs_sem.at[i]).wait()
    for k in range(1, Z):
        give_grad(k).wait_send()
    for swap in (swap2, swap1, cross, swap3, swap4):
        swap.wait_send()
    local(second_in, second_in, px_sem.at[2]).wait()
    local(column_in, column_in, px_sem.at[6]).wait()
    local(first_in, first_in, px_sem.at[8]).wait()
    local(everyone_in, everyone_in, px_sem.at[10]).wait()


def on_device(dims, features, adjacency_one, pre_hidden, adjacency_two, weight_two, out_grad):
    Y, X, Z, G, C = dims
    NP, ZZ = Y * X, Z * G
    cw, nb = features.shape[2:]
    relations, word_rows = adjacency_one.shape[2:4]
    dst, h = pre_hidden.shape[2:]
    seeds = out_grad.shape[2]
    half = (relations + 1) // C
    hc = h // NP
    rows2 = half * hc + 8
    factor = float(seeds * NP * ZZ * C) ** (-0.5)
    vmem = pltpu.VMEM
    any_spec = pl.BlockSpec(memory_space=pl.ANY)
    vmem_spec = pl.BlockSpec(memory_space=pltpu.VMEM)
    dma = pltpu.SemaphoreType.DMA
    out1, out2, outb = pl.pallas_call(
        functools.partial(kernel, dims, factor),
        name="graph_grads",
        out_shape=(
            jax.ShapeDtypeStruct((relations + 1, cw, h), F32),
            jax.ShapeDtypeStruct((relations + 1, h, h), F32),
            jax.ShapeDtypeStruct((8, h), F32),
        ),
        in_specs=[any_spec] * 6,
        out_specs=(vmem_spec,) * 3,
        scratch_shapes=[
            vmem((dst, h), BF16),
            vmem(adjacency_two.shape[2:], jnp.int32),
            vmem(weight_two.shape, BF16),
            vmem((seeds, h), BF16),
            vmem((Z * relations, word_rows, nb), jnp.int32),
            vmem((relations, seeds, dst), BF16),
            vmem((Z * relations, dst, nb), BF16),
            vmem((Z * relations, 8, dst), F32),
            vmem((Z, NP * cw, nb), BF16),
            vmem((Z, dst, h), BF16),
            vmem((dst, h), F32),
            vmem((relations + 1, NP * cw, h), F32),
            vmem((relations + 1, h, h), F32),
            vmem((half * h + 8, h), BF16),
            vmem((half * h + 8, h), BF16),
            vmem((NP, rows2, h), BF16),
            vmem((NP, rows2, h), BF16),
            vmem((ZZ, rows2, h), BF16),
            vmem((NP, rows2, h), BF16),
            vmem((NP, rows2, h), BF16),
            vmem((half, NP * cw, h), BF16),
            vmem((half, NP * cw, h), BF16),
            vmem((NP, half * cw, h), BF16),
            vmem((NP, half * cw, h), BF16),
            vmem((half * cw, h), BF16),
            vmem((half * cw, h), BF16),
            vmem((half, cw, h), F32),
            vmem((half, cw, h), F32),
            dma((4 + Z,)),
            dma((Z,)),
            dma((Z,)),
            dma((Z,)),
            dma((Z,)),
            dma((Z,)),
            dma((18,)),
        ],
        compiler_params=pltpu.CompilerParams(
            collective_id=0, has_side_effects=True, vmem_limit_bytes=48 * 2**20
        ),
    )(features, adjacency_one, pre_hidden, adjacency_two, weight_two, out_grad)
    return out1, outb[0], out2, outb[1]


def build(devices, dims):
    torus = Mesh(devices.reshape(dims), AXES)
    placed = (
        P(REP, None, FEAT, None),
        P(REP, None, None, None, None),
        P(REP, FEAT, None, None),
        P(REP, FEAT, None, None, None),
        P(),
        P(REP, FEAT, None, None),
    )
    return jax.shard_map(
        functools.partial(on_device, dims),
        mesh=torus,
        in_specs=placed,
        out_specs=(P(None, FEAT, None), P(), P(), P()),
        check_vma=False,
    )


def solution(mesh):
    dims = (4, 4, mesh.shape["feat"] // 16, mesh.shape["rep"] // 2, 2)
    return build(mesh.devices, dims)
```

```python
import functools
import types

import jax
import jax.numpy as jnp
from jax import lax
from jax.experimental import pallas as pl
from jax.experimental.pallas import tpu as pltpu
from jax.sharding import Mesh
from jax.sharding import PartitionSpec as P

MESH = pl.DeviceIdType.MESH
AXES = ("y", "x", "z", "g", "c")
FEAT = ("y", "x", "z")
REP = ("g", "c")
BF16 = jnp.bfloat16
F32 = jnp.float32
NN = (((1,), (0,)), ((), ()))
NT = (((1,), (1,)), ((), ()))
TN = (((0,), (0,)), ((), ()))
TOP = 16
BIAS = 8
SWAP2, RS2, COL, AG, SWAP3, SWAP1, RS1, CROSS, SWAP4 = range(9)


def mm(a, b, dims):
    return lax.dot_general(a, b, dims, preferred_element_type=F32)


def local(src, dst, sem):
    return pltpu.make_async_copy(src, dst, sem)


def remote(src, dst, send, recv, device):
    return pltpu.make_async_remote_copy(
        src_ref=src, dst_ref=dst, send_sem=send, recv_sem=recv, device_id=device, device_id_type=MESH
    )


def spread_bits(words, r, out, rows, width):
    shift = lax.broadcasted_iota(jnp.int32, (16, width), 0)
    for w in range(rows // 16):
        word = jnp.broadcast_to(words[r, pl.ds(w, 1), :], (16, width))
        bits = lax.bitwise_and(lax.shift_right_logical(word, shift), 1)
        out[r, pl.ds(16 * w, 16), :] = bits.astype(F32).astype(BF16)


def spread_scaled(words, t, out, rows, width):
    mask = lax.shift_left(1, lax.broadcasted_iota(jnp.int32, (16, width), 0))
    for w in range(rows // 16):
        word = jnp.broadcast_to(words[t, pl.ds(w, 1), :], (16, width))
        out[t, pl.ds(16 * w, 16), :] = lax.bitwise_and(word, mask).astype(F32).astype(BF16)


def skip_loop(count, skipped, body):
    def step(t, carry):
        body(t)
        return carry

    lax.fori_loop(0, skipped, step, 0)
    if skipped + 1 < count:
        lax.fori_loop(skipped + 1, count, step, 0)


def kernel(dims, factor, names, feat, adj1, pre_any, adj2, w2_any, og_any, out1, out2, outb, *scratch):
    v = types.SimpleNamespace(**dict(zip(names, scratch)))
    Y, X, Z, G, C = dims
    NP, ZZ = Y * X, Z * G
    y, x, z, g, c = (lax.axis_index(a) for a in AXES)
    me = y * X + x
    zabs = g * Z + z
    relations = v.words1.shape[0] // Z
    half = (relations + 1) // C
    cw = feat.shape[2]
    seeds, h = v.og.shape
    dst = v.pre.shape[0]
    hc = h // NP
    base = me * Z
    partner = (y, x, z, g, 1 - c)
    across = (y, x, z, 1 - g, c)

    def send_sem(phase, q=0):
        return v.ss.at[phase * half + q]

    def recv_sem(phase, q=0):
        return v.rs.at[phase * half + q]

    def over_plane(body, sign=1):
        def step(t):
            dy = lax.rem(Y // 2 + lax.div(t, X), Y)
            dx = lax.rem(X // 2 + lax.rem(t, X), X)
            yy = lax.rem(y + sign * dy + Y, Y)
            xx = lax.rem(x + sign * dx + X, X)
            body(dy * X + dx, yy * X + xx, (yy, xx, z, g, c))

        skip_loop(NP, (Y - Y // 2) * X + X - X // 2 if X > 1 else Y - Y // 2, step)

    def over_column(body):
        def step(t):
            zz = lax.rem(zabs + ZZ // 2 + t, ZZ)
            body((y, x, lax.rem(zz, Z), lax.div(zz, Z), c))

        skip_loop(ZZ, ZZ - ZZ // 2, step)

    def minibatch(i):
        return lax.rem(z + i, 2) + 2 * lax.rem(lax.div(z, 2) + i // 2 if isinstance(i, int) else lax.div(z, 2) + lax.div(i, 2), 2)

    barrier = pltpu.get_barrier_semaphore()

    def greet(device):
        pl.semaphore_signal(barrier, inc=1, device_id=device, device_id_type=MESH)

    over_plane(lambda slot, other, device: greet(device))
    over_column(greet)
    greet(partner)

    loads = [
        local(adj2.at[0, 0], v.words2, v.loc.at[0]),
        local(pre_any.at[0, 0], v.pre, v.loc.at[1]),
        local(og_any.at[0, 0], v.og, v.loc.at[2]),
        local(w2_any, v.w2, v.loc.at[3]),
        local(feat.at[0], v.xv, v.loc.at[4]),
    ]
    for q in range(Z):
        loads.append(
            local(adj1.at[0, base + q], v.words1.at[pl.ds(q * relations, relations)], v.loc.at[5 + q])
        )
    for load in loads:
        load.start()
    v.rx[:, pl.ds(0, TOP), :] = jnp.ones((Z, TOP, v.rx.shape[2]), BF16)
    loads[0].wait()
    for r in range(relations):
        spread_bits(v.words2, r, v.dense2, seeds, h)

    for load in loads[1:4]:
        load.wait()
    hidden = jnp.maximum(v.pre[...], 0)
    scaled = v.og[...].astype(F32) * factor
    low = scaled.astype(BF16)
    ones = jnp.ones((h, h), BF16)
    v.wg[0] = mm(hidden[:seeds], low, TN)
    v.total[...] = jnp.zeros_like(v.total)
    v.total[pl.ds(0, seeds), :] = mm(low, v.w2[0], NT)
    for r in range(relations):
        dense = v.dense2[r]
        inverse = 1.0 / jnp.maximum(mm(dense, ones, NN), 1.0)
        mixed = (mm(dense, hidden, NN) * inverse).astype(BF16)
        v.wg[r + 1] = mm(mixed, low, TN)
        backed = (mm(low, v.w2[r + 1], NT) * inverse).astype(BF16)
        v.total[...] += mm(dense, backed, TN)
    grad = jnp.where(v.pre[...] > 0, v.total[...], 0.0).astype(BF16)
    v.hgown[...] = grad
    local(v.hgown, v.hgbuf.at[z], v.hr.at[0]).start()
    row = lax.broadcasted_iota(jnp.int32, (BIAS, h), 0)
    bias_one = jnp.sum(grad.astype(F32), axis=0, keepdims=True)
    bias_two = jnp.sum(scaled, axis=0, keepdims=True)
    first = c == 0
    bias_keep = jnp.where(row == 0, jnp.where(first, bias_one, bias_two), 0.0)
    bias_give = jnp.where(row == 0, jnp.where(first, bias_two, bias_one), 0.0)
    for q in range(half):
        v.cxs2[pl.ds(q * h, h), :] = v.wg[(1 - c) * half + q].astype(BF16)
    v.cxs2[pl.ds(half * h, BIAS), :] = bias_give.astype(BF16)
    loads[4].wait()

    pl.semaphore_wait(barrier, NP + ZZ - 1)

    swap2 = remote(v.cxs2, v.cxr2, send_sem(SWAP2), recv_sem(SWAP2), partner)
    swap2.start()

    def give_grad(k):
        return remote(v.hgown, v.hgbuf.at[z], v.hs.at[k], v.hr.at[k], (y, x, minibatch(k), g, c))

    for k in range(1, Z):
        give_grad(k).start()

    for i in range(Z):
        m = minibatch(i)
        local(v.xv.at[base + m], v.rx.at[m, pl.ds(TOP, cw), :], v.own.at[i]).start()
        over_plane(
            lambda slot, other, device: remote(
                v.xv.at[other * Z + m],
                v.rx.at[m, pl.ds(pl.multiple_of(TOP + slot * cw, cw), cw), :],
                v.xs.at[i],
                v.xr.at[i],
                device,
            ).start()
        )

    for load in loads[5:]:
        load.wait()

    def spread_one(t, carry):
        spread_scaled(v.words1, t, v.dense1, 16 * v.words1.shape[1], v.words1.shape[2])
        return carry

    lax.fori_loop(0, Z * relations, spread_one, 0)

    swap2.wait_recv()
    bias = (bias_keep + v.cxr2[pl.ds(half * h, BIAS), :].astype(F32)).astype(BF16)
    v.s2_0[:, pl.ds(hc, BIAS), :] = jnp.broadcast_to(bias[None], (NP, BIAS, h))
    s2 = [getattr(v, f"s2_{q}") for q in range(half)]
    r2 = [getattr(v, f"r2_{q}") for q in range(half)]
    zb = [getattr(v, f"zb_{q}") for q in range(half)]
    ag = [getattr(v, f"ag_{q}") for q in range(half)]
    agp = [getattr(v, f"agp_{q}") for q in range(half)]
    for q in range(half):
        both = v.wg[c * half + q] + v.cxr2[pl.ds(q * h, h), :].astype(F32)
        s2[q][:, pl.ds(0, hc), :] = both.astype(BF16).reshape(NP, hc, h)
        over_plane(
            lambda slot, other, device: remote(
                s2[q].at[other], r2[q].at[slot], send_sem(RS2, q), recv_sem(RS2, q), device
            ).start()
        )

    v.acc[...] = jnp.zeros_like(v.acc)
    least = lax.shift_left(1, lax.rem(lax.broadcasted_iota(jnp.int32, (1, dst), 1), 16)).astype(F32)

    def one_minibatch(i, carry):
        m = minibatch(i)
        local(v.xv.at[base + m], v.rx.at[m, pl.ds(TOP, cw), :], v.own.at[i]).wait()
        arrived = v.rx.at[m, pl.ds(TOP + cw, (NP - 1) * cw), :]
        local(arrived, arrived, v.xr.at[i]).wait()
        local(v.hgown, v.hgbuf.at[m], v.hr.at[i]).wait()
        grad_m = v.hgbuf[m]
        v.acc[0] += mm(v.rx[m, pl.ds(TOP, NP * cw), pl.ds(0, dst)], grad_m, NN)
        for r in range(relations):
            product = mm(v.rx[m], v.dense1[m * relations + r], NT)
            weight = 1.0 / jnp.maximum(product[:1], least)
            v.gathered[r] = (product[TOP:] * weight).astype(BF16)
        for r in range(relations):
            v.acc[r + 1] += mm(v.gathered[r], grad_m, NN)
        return carry

    lax.fori_loop(0, Z, one_minibatch, 0)

    def swap1(q):
        return remote(v.cxs1.at[q], v.cxr1.at[q], send_sem(SWAP1, q), recv_sem(SWAP1, q), partner)

    for q in range(half):
        v.cxs1[q] = v.acc[(1 - c) * half + q].astype(BF16)
        swap1(q).start()

    def second_sum(q):
        arrived = r2[q].at[pl.ds(1, NP - 1)]
        local(arrived, arrived, recv_sem(RS2, q)).wait()
        summed = s2[q][me].astype(F32)
        for k in range(1, NP):
            summed += r2[q][k].astype(F32)
        zb[q][zabs] = summed.astype(BF16)
        over_column(
            lambda device: remote(
                zb[q].at[zabs], zb[q].at[zabs], send_sem(COL, q), recv_sem(COL, q), device
            ).start()
        )

    def column_sum(q):
        arrived = zb[q].at[pl.ds(0, ZZ - 1)]
        local(arrived, arrived, recv_sem(COL, q)).wait()
        summed = zb[q][0].astype(F32)
        for k in range(1, ZZ):
            summed += zb[q][k].astype(F32)
        ag[q][me] = summed.astype(BF16)
        over_plane(
            lambda slot, other, device: remote(
                ag[q].at[me], ag[q].at[me], send_sem(AG, q), recv_sem(AG, q), device
            ).start()
        )

    second_sum(0)

    for q in range(half):
        swap1(q).wait_recv()
        both = v.acc[c * half + q] + v.cxr1[q].astype(F32)
        v.s1[q] = both.astype(BF16).reshape(NP, cw, h)
        over_plane(
            lambda slot, other, device: remote(
                v.s1.at[q, slot], v.r1.at[q, slot], send_sem(RS1, q), recv_sem(RS1, q), device
            ).start(),
            -1,
        )

    for q in range(1, half):
        second_sum(q)

    for q in range(half):
        column_sum(q)

    for q in range(half):
        arrived = v.r1.at[q, pl.ds(1, NP - 1)]
        local(arrived, arrived, recv_sem(RS1, q)).wait()
        summed = v.s1[q, 0].astype(F32)
        for k in range(1, NP):
            summed += v.r1[q, k].astype(F32)
        v.zhs[q] = summed.astype(BF16)
    cross = remote(v.zhs, v.zhr, send_sem(CROSS), recv_sem(CROSS), across)
    cross.start()

    def swap3(q):
        return remote(ag[q], agp[q], send_sem(SWAP3, q), recv_sem(SWAP3, q), partner)

    stores = []

    def store(src, dst_ref):
        stores.append(local(src, dst_ref, v.st.at[len(stores)]))
        stores[-1].start()

    for q in range(half):
        arrived = ag[q].at[pl.ds(0, NP - 1)]
        local(arrived, arrived, recv_sem(AG, q)).wait()
        swap3(q).start()
        store(ag[q].at[:, pl.ds(0, hc), :], out2.at[c * half + q])

    cross.wait_recv()
    v.d1s[...] = v.zhs[...].astype(F32) + v.zhr[...].astype(F32)
    swap4 = remote(v.d1s, v.d1r, send_sem(SWAP4), recv_sem(SWAP4), partner)
    swap4.start()
    store(v.d1s, out1.at[pl.ds(c * half, half)])

    for q in range(half):
        swap3(q).wait_recv()
        store(agp[q].at[:, pl.ds(0, hc), :], out2.at[(1 - c) * half + q])
        if q == 0:
            kept = ag[0][0, pl.ds(hc, BIAS), :].astype(F32)[:1]
            given = agp[0][0, pl.ds(hc, BIAS), :].astype(F32)[:1]
            v.bias[...] = jnp.where(row == c, kept, given)
            store(v.bias, outb)

    swap4.wait_recv()
    store(v.d1r, out1.at[pl.ds((1 - c) * half, half)])

    for i in range(Z):
        sent = v.xv.at[pl.ds(0, NP - 1)]
        local(sent, sent, v.xs.at[i]).wait()
    for k in range(1, Z):
        give_grad(k).wait_send()
    for swap in (swap2, cross, swap4):
        swap.wait_send()
    for q in range(half):
        swap1(q).wait_send()
        swap3(q).wait_send()
        for phase, ref in (
            (RS2, r2[q].at[pl.ds(1, NP - 1)]),
            (COL, zb[q].at[pl.ds(0, ZZ - 1)]),
            (AG, ag[q].at[pl.ds(0, NP - 1)]),
            (RS1, v.r1.at[q, pl.ds(1, NP - 1)]),
        ):
            local(ref, ref, send_sem(phase, q)).wait()
    for copy in stores:
        copy.wait()


def on_device(dims, features, adjacency_one, pre_hidden, adjacency_two, weight_two, out_grad):
    Y, X, Z, G, C = dims
    NP, ZZ = Y * X, Z * G
    blocks, cw, nb = features.shape[1:]
    relations, word_rows = adjacency_one.shape[2:4]
    dst, h = pre_hidden.shape[2:]
    seeds = out_grad.shape[2]
    half = (relations + 1) // C
    hc = h // NP
    factor = float(seeds * NP * ZZ * C) ** (-0.5)
    vmem = pltpu.VMEM
    any_spec = pl.BlockSpec(memory_space=pl.ANY)
    dma = pltpu.SemaphoreType.DMA
    shapes = dict(
        pre=vmem((dst, h), BF16),
        words2=vmem(adjacency_two.shape[2:], jnp.int32),
        w2=vmem(weight_two.shape, BF16),
        og=vmem((seeds, h), BF16),
        xv=vmem((blocks, cw, nb), BF16),
        words1=vmem((Z * relations, word_rows, nb), jnp.int32),
        dense2=vmem((relations, seeds, dst), BF16),
        dense1=vmem((Z * relations, dst, nb), BF16),
        rx=vmem((Z, TOP + NP * cw, nb), BF16),
        hgown=vmem((dst, h), BF16),
        hgbuf=vmem((Z, dst, h), BF16),
        gathered=vmem((relations, NP * cw, dst), BF16),
        total=vmem((dst, h), F32),
        acc=vmem((relations + 1, NP * cw, h), F32),
        wg=vmem((relations + 1, h, h), F32),
        cxs2=vmem((half * h + BIAS, h), BF16),
        cxr2=vmem((half * h + BIAS, h), BF16),
        cxs1=vmem((half, NP * cw, h), BF16),
        cxr1=vmem((half, NP * cw, h), BF16),
        s1=vmem((half, NP, cw, h), BF16),
        r1=vmem((half, NP, cw, h), BF16),
        zhs=vmem((half, cw, h), BF16),
        zhr=vmem((half, cw, h), BF16),
        d1s=vmem((half, cw, h), F32),
        d1r=vmem((half, cw, h), F32),
        bias=vmem((BIAS, h), F32),
        loc=dma((5 + Z,)),
        own=dma((Z,)),
        xs=dma((Z,)),
        xr=dma((Z,)),
        hs=dma((Z,)),
        hr=dma((Z,)),
        ss=dma((9 * half,)),
        rs=dma((9 * half,)),
        st=dma((2 * half + 3,)),
    )
    for q in range(half):
        rows = hc + (BIAS if q == 0 else 0)
        for name in ("s2", "r2", "ag", "agp"):
            shapes[f"{name}_{q}"] = vmem((NP, rows, h), BF16)
        shapes[f"zb_{q}"] = vmem((ZZ, rows, h), BF16)
    out1, out2, outb = pl.pallas_call(
        functools.partial(kernel, dims, factor, tuple(shapes)),
        name="graph_grads",
        out_shape=(
            jax.ShapeDtypeStruct((relations + 1, cw, h), F32),
            jax.ShapeDtypeStruct((relations + 1, NP, hc, h), BF16),
            jax.ShapeDtypeStruct((BIAS, h), F32),
        ),
        in_specs=[any_spec] * 6,
        out_specs=(any_spec,) * 3,
        scratch_shapes=list(shapes.values()),
        compiler_params=pltpu.CompilerParams(
            collective_id=0, has_side_effects=True, vmem_limit_bytes=66000000
        ),
    )(features, adjacency_one, pre_hidden, adjacency_two, weight_two, out_grad)
    return out1, outb[0], out2.reshape(relations + 1, h, h).astype(F32), outb[1]


def build(devices, dims):
    torus = Mesh(devices.reshape(dims), AXES)
    placed = (
        P(REP, None, FEAT, None),
        P(REP, None, None, None, None),
        P(REP, FEAT, None, None),
        P(REP, FEAT, None, None, None),
        P(),
        P(REP, FEAT, None, None),
    )
    return jax.shard_map(
        functools.partial(on_device, dims),
        mesh=torus,
        in_specs=placed,
        out_specs=(P(None, FEAT, None), P(), P(), P()),
        check_vma=False,
    )


def solution(mesh):
    dims = (4, 4, mesh.shape["feat"] // 16, mesh.shape["rep"] // 2, 2)
    return build(mesh.devices, dims)
```

```python
import functools
import types

import jax
import jax.numpy as jnp
from jax import lax
from jax.experimental import pallas as pl
from jax.experimental.pallas import tpu as pltpu
from jax.sharding import Mesh
from jax.sharding import PartitionSpec as P

MESH = pl.DeviceIdType.MESH
AXES = ("y", "x", "z", "g", "c")
FEAT = ("y", "x", "z")
REP = ("g", "c")
BF16 = jnp.bfloat16
F32 = jnp.float32
NN = (((1,), (0,)), ((), ()))
NT = (((1,), (1,)), ((), ()))
TN = (((0,), (0,)), ((), ()))
WIDEN_LIMIT = 66000000
MAIN_LIMIT = 66000000
TOP = 16
PARTS = 1
PHASES = 13
SWAP2, RS2, COL, AG, SWAP3, SWAP1, RS1, CROSS, SWAP4, BSWAP, BPLANE, BCOL, BLAST = range(PHASES)


def mm(a, b, dims):
    return lax.dot_general(a, b, dims, preferred_element_type=F32)


def local(src, dst, sem):
    return pltpu.make_async_copy(src, dst, sem)


def remote(src, dst, send, recv, device):
    return pltpu.make_async_remote_copy(
        src_ref=src, dst_ref=dst, send_sem=send, recv_sem=recv, device_id=device, device_id_type=MESH
    )


def spread_bits(words, r, out, rows, width):
    shift = lax.broadcasted_iota(jnp.int32, (16, width), 0)
    for w in range(rows // 16):
        word = jnp.broadcast_to(words[r, pl.ds(w, 1), :], (16, width))
        bits = lax.bitwise_and(lax.shift_right_logical(word, shift), 1)
        out[r, pl.ds(16 * w, 16), :] = bits.astype(F32).astype(BF16)


def spread_scaled(words, t, out, rows, width):
    mask = lax.shift_left(1, lax.broadcasted_iota(jnp.int32, (16, width), 0))
    for w in range(rows // 16):
        word = jnp.broadcast_to(words[t, pl.ds(w, 1), :], (16, width))
        out[t, pl.ds(16 * w, 16), :] = lax.bitwise_and(word, mask).astype(F32).astype(BF16)


def skip_loop(count, skipped, body):
    def step(t, carry):
        body(t)
        return carry

    lax.fori_loop(0, skipped, step, 0)
    if skipped + 1 < count:
        lax.fori_loop(skipped + 1, count, step, 0)


def kernel(dims, factor, names, feat, adj1, pre_any, adj2, w2_any, og_any, out1, out2, outb, *scratch):
    v = types.SimpleNamespace(**dict(zip(names, scratch)))
    Y, X, Z, G, C = dims
    NP, ZZ = Y * X, Z * G
    y, x, z, g, c = (lax.axis_index(a) for a in AXES)
    me = y * X + x
    zabs = g * Z + z
    relations = v.words1.shape[0] // Z
    half = (relations + 1) // C
    cw = feat.shape[2]
    seeds, h = v.og.shape
    dst = v.pre.shape[0]
    hc = h // NP
    chunks = [(q, p) for q in range(half) for p in range(PARTS)]
    pc = hc // PARTS
    base = me * Z
    partner = (y, x, z, g, 1 - c)
    across = (y, x, z, 1 - g, c)

    def send_sem(phase, q=0):
        return v.ss.at[phase * len(chunks) + q]

    def recv_sem(phase, q=0):
        return v.rs.at[phase * len(chunks) + q]

    rows_of = [lax.rem(y + d, Y) for d in range(Y)]
    cols_of = [lax.rem(x + d, X) for d in range(X)]
    pairs = [(dy, dx) for dy in range(Y) for dx in range(X) if dy or dx]
    pairs.sort(key=lambda p: -min(p[0], Y - p[0]) - min(p[1], X - p[1]))

    def over_plane(body, sign=1):
        for dy, dx in pairs:
            yy, xx = rows_of[(sign * dy) % Y], cols_of[(sign * dx) % X]
            body(dy * X + dx, yy * X + xx, (yy, xx, z, g, c))

    def over_column(body):
        def step(t):
            zz = lax.rem(zabs + ZZ // 2 + t, ZZ)
            body((y, x, lax.rem(zz, Z), lax.div(zz, Z), c))

        skip_loop(ZZ, ZZ - ZZ // 2, step)

    def minibatch(i):
        return lax.rem(z + i, 2) + 2 * lax.rem(lax.div(z, 2) + i // 2 if isinstance(i, int) else lax.div(z, 2) + lax.div(i, 2), 2)

    barrier = pltpu.get_barrier_semaphore()

    def greet(device):
        pl.semaphore_signal(barrier, inc=1, device_id=device, device_id_type=MESH)

    over_plane(lambda slot, other, device: greet(device))
    over_column(greet)
    greet(partner)

    loads = [
        local(adj2.at[0, 0], v.words2, v.loc.at[0]),
        local(pre_any.at[0, 0], v.pre, v.loc.at[1]),
        local(og_any.at[0, 0], v.og, v.loc.at[2]),
        local(w2_any, v.w2, v.loc.at[3]),
        local(feat.at[0], v.xv, v.loc.at[4]),
    ]
    for q in range(Z):
        loads.append(
            local(adj1.at[0, base + q], v.words1.at[pl.ds(q * relations, relations)], v.loc.at[5 + q])
        )
    for load in loads:
        load.start()
    v.rx[:, pl.ds(0, TOP), :] = jnp.ones((Z, TOP, v.rx.shape[2]), BF16)
    loads[0].wait()
    for r in range(relations):
        spread_bits(v.words2, r, v.dense2, seeds, h)

    for load in loads[1:4]:
        load.wait()
    scaled = v.og[...].astype(F32) * factor
    low = scaled.astype(BF16)
    ones = jnp.ones((h, h), BF16)
    v.total[...] = jnp.zeros_like(v.total)
    v.total[pl.ds(0, seeds), :] = mm(low, v.w2[0], NT)
    for r in range(relations):
        inverse = 1.0 / jnp.maximum(mm(v.dense2[r], ones, NN), 1.0)
        v.weight2[r] = inverse
        backed = (mm(low, v.w2[r + 1], NT) * inverse).astype(BF16)
        v.total[...] += mm(v.dense2[r], backed, TN)
    v.hgown[...] = jnp.where(v.pre[...] > 0, v.total[...], 0.0).astype(BF16)
    local(v.hgown, v.hgbuf.at[z], v.hr.at[0]).start()
    loads[4].wait()

    pl.semaphore_wait(barrier, NP + ZZ - 1)

    def give_grad(k):
        return remote(v.hgown, v.hgbuf.at[z], v.hs.at[k], v.hr.at[k], (y, x, minibatch(k), g, c))

    for k in range(1, Z):
        give_grad(k).start()

    def send_features(i, carry):
        m = minibatch(i)
        local(v.xv.at[base + m], v.rx.at[m, pl.ds(TOP, cw), :], v.own.at[i]).start()
        over_plane(
            lambda slot, other, device: remote(
                v.xv.at[other * Z + m],
                v.rx.at[m, pl.ds(TOP + slot * cw, cw), :],
                v.xs.at[i],
                v.xr.at[i],
                device,
            ).start()
        )
        return carry

    lax.fori_loop(0, Z, send_features, 0)

    hidden = jnp.maximum(v.pre[...], 0)
    scaled = v.og[...].astype(F32) * factor
    low = scaled.astype(BF16)
    v.wg[0] = mm(hidden[:seeds], low, TN)
    for r in range(relations):
        mixed = (mm(v.dense2[r], hidden, NN) * v.weight2[r]).astype(BF16)
        v.wg[r + 1] = mm(mixed, low, TN)
    bias_one = jnp.sum(v.hgown[...].astype(F32), axis=0, keepdims=True)
    bias_two = jnp.sum(scaled, axis=0, keepdims=True)
    first = c == 0
    bias_keep = jnp.where(first, bias_one, bias_two)
    v.bs[...] = jnp.where(first, bias_two, bias_one)
    for q in range(half):
        v.cxs2[pl.ds(q * h, h), :] = v.wg[(1 - c) * half + q].astype(BF16)
    swap2 = remote(v.cxs2, v.cxr2, send_sem(SWAP2), recv_sem(SWAP2), partner)
    swap2.start()
    bias_swap = remote(v.bs, v.br, send_sem(BSWAP), recv_sem(BSWAP), partner)
    bias_swap.start()

    for load in loads[5:]:
        load.wait()

    def spread_one(t, carry):
        spread_scaled(v.words1, t, v.dense1, 16 * v.words1.shape[1], v.words1.shape[2])
        return carry

    lax.fori_loop(0, Z * relations, spread_one, 0)

    bias_swap.wait_recv()
    v.bplane[me] = bias_keep + v.br[...]
    over_plane(
        lambda slot, other, device: remote(
            v.bplane.at[me], v.bplane.at[me], send_sem(BPLANE), recv_sem(BPLANE), device
        ).start()
    )
    s2 = [getattr(v, f"s2_{n}") for n in range(len(chunks))]
    r2 = [getattr(v, f"r2_{n}") for n in range(len(chunks))]
    zb = [getattr(v, f"zb_{n}") for n in range(len(chunks))]
    ag = [getattr(v, f"ag_{n}") for n in range(len(chunks))]
    swap2.wait_recv()
    for n, (q, p) in enumerate(chunks):
        if p == 0:
            both = (v.wg[c * half + q] + v.cxr2[pl.ds(q * h, h), :].astype(F32)).astype(BF16).reshape(NP, hc, h)
        s2[n][...] = both[:, p * pc : (p + 1) * pc]
        over_plane(
            lambda slot, other, device: remote(
                s2[n].at[other], r2[n].at[slot], send_sem(RS2, n), recv_sem(RS2, n), device
            ).start()
        )

    v.acc[...] = jnp.zeros_like(v.acc)
    least = lax.shift_left(1, lax.rem(lax.broadcasted_iota(jnp.int32, (1, dst), 1), 16)).astype(F32)

    def one_minibatch(i, carry):
        m = minibatch(i)
        local(v.xv.at[base + m], v.rx.at[m, pl.ds(TOP, cw), :], v.own.at[i]).wait()
        arrived = v.rx.at[m, pl.ds(TOP + cw, (NP - 1) * cw), :]
        local(arrived, arrived, v.xr.at[i]).wait()
        local(v.hgown, v.hgbuf.at[m], v.hr.at[i]).wait()
        grad_m = v.hgbuf[m]
        v.acc[0] += mm(v.rx[m, pl.ds(TOP, NP * cw), pl.ds(0, dst)], grad_m, NN)
        for r in range(relations):
            product = mm(v.rx[m], v.dense1[m * relations + r], NT)
            weight = 1.0 / jnp.maximum(product[:1], least)
            v.gathered[r] = (product[TOP:] * weight).astype(BF16)
        for r in range(relations):
            v.acc[r + 1] += mm(v.gathered[r], grad_m, NN)
        return carry

    lax.fori_loop(0, Z, one_minibatch, 0)

    def swap1(q):
        return remote(v.cxs1.at[q], v.cxr1.at[q], send_sem(SWAP1, q), recv_sem(SWAP1, q), partner)

    for q in range(half):
        v.cxs1[q] = v.acc[(1 - c) * half + q].astype(BF16)
        swap1(q).start()

    def second_sum(q):
        arrived = r2[q].at[pl.ds(1, NP - 1)]
        local(arrived, arrived, recv_sem(RS2, q)).wait()
        summed = s2[q][me].astype(F32)
        for k in range(1, NP):
            summed += r2[q][k].astype(F32)
        zb[q][zabs] = summed.astype(BF16)
        over_column(
            lambda device: remote(
                zb[q].at[zabs], zb[q].at[zabs], send_sem(COL, q), recv_sem(COL, q), device
            ).start()
        )

    def column_sum(q):
        arrived = zb[q].at[pl.ds(0, ZZ - 1)]
        local(arrived, arrived, recv_sem(COL, q)).wait()
        summed = zb[q][0].astype(F32)
        for k in range(1, ZZ):
            summed += zb[q][k].astype(F32)
        ag[q][me] = summed.astype(BF16)
        over_plane(
            lambda slot, other, device: remote(
                ag[q].at[me], ag[q].at[me], send_sem(AG, q), recv_sem(AG, q), device
            ).start()
        )

    for q in range(half):
        swap1(q).wait_recv()
        both = v.acc[c * half + q] + v.cxr1[q].astype(F32)
        v.s1[:, pl.ds(q * cw, cw), :] = both.astype(BF16).reshape(NP, cw, h)
    over_plane(
        lambda slot, other, device: remote(
            v.s1.at[slot], v.r1.at[slot], send_sem(RS1), recv_sem(RS1), device
        ).start(),
        -1,
    )

    for n in range(len(chunks)):
        second_sum(n)
    bias_in = v.bplane.at[pl.ds(0, NP - 1)]
    local(bias_in, bias_in, recv_sem(BPLANE)).wait()
    v.bcol[zabs] = jnp.sum(v.bplane[...], axis=0)
    over_column(
        lambda device: remote(
            v.bcol.at[zabs], v.bcol.at[zabs], send_sem(BCOL), recv_sem(BCOL), device
        ).start()
    )

    for n in range(len(chunks)):
        column_sum(n)

    first_in = v.r1.at[pl.ds(1, NP - 1)]
    local(first_in, first_in, recv_sem(RS1)).wait()
    summed = v.s1[0].astype(F32)
    for k in range(1, NP):
        summed += v.r1[k].astype(F32)
    v.zhs[...] = summed.astype(BF16).reshape(half, cw, h)
    cross = remote(v.zhs, v.zhr, send_sem(CROSS), recv_sem(CROSS), across)
    cross.start()
    bias_col = v.bcol.at[pl.ds(0, ZZ - 1)]
    local(bias_col, bias_col, recv_sem(BCOL)).wait()
    v.bmine[...] = jnp.sum(v.bcol[...], axis=0)
    bias_last = remote(v.bmine, v.btheirs, send_sem(BLAST), recv_sem(BLAST), partner)
    bias_last.start()

    def panel_part(n):
        q, p = chunks[n]
        return out2.at[c * half + q, :, pl.ds(p * pc, pc), :]

    def swap3(n):
        return remote(ag[n], panel_part(n), send_sem(SWAP3, n), recv_sem(SWAP3, n), partner)

    stores = []

    def store(src, dst_ref):
        stores.append(local(src, dst_ref, v.st.at[len(stores)]))
        stores[-1].start()

    for n in range(len(chunks)):
        arrived = ag[n].at[pl.ds(0, NP - 1)]
        local(arrived, arrived, recv_sem(AG, n)).wait()
        swap3(n).start()
        store(ag[n], panel_part(n))

    cross.wait_recv()
    v.d1s[...] = v.zhs[...].astype(F32) + v.zhr[...].astype(F32)
    swap4 = remote(v.d1s, out1.at[pl.ds(c * half, half)], send_sem(SWAP4), recv_sem(SWAP4), partner)
    swap4.start()
    store(v.d1s, out1.at[pl.ds(c * half, half)])

    bias_last.wait_recv()
    mine, theirs = v.bmine[...], v.btheirs[...]
    row = lax.broadcasted_iota(jnp.int32, (8, h), 0)
    v.bias[...] = jnp.where(row == c, mine, theirs)
    store(v.bias, outb)

    for n in range(len(chunks)):
        swap3(n).wait_recv()

    swap4.wait_recv()

    for i in range(Z):
        sent = v.xv.at[pl.ds(0, NP - 1)]
        local(sent, sent, v.xs.at[i]).wait()
    for k in range(1, Z):
        give_grad(k).wait_send()
    for swap in (swap2, cross, swap4, bias_swap, bias_last):
        swap.wait_send()
    for q in range(half):
        swap1(q).wait_send()
    for n in range(len(chunks)):
        swap3(n).wait_send()
        for phase, ref in (
            (RS2, r2[n].at[pl.ds(1, NP - 1)]),
            (COL, zb[n].at[pl.ds(0, ZZ - 1)]),
            (AG, ag[n].at[pl.ds(0, NP - 1)]),
        ):
            local(ref, ref, send_sem(phase, n)).wait()
    local(bias_in, bias_in, send_sem(BPLANE)).wait()
    local(bias_col, bias_col, send_sem(BCOL)).wait()
    local(first_in, first_in, send_sem(RS1)).wait()
    for copy in stores:
        copy.wait()


def widen(first_in, second_in, bias_in, first, second, bias_one, bias_two, one, low, wide, bias, come, go):
    panels = low.shape[0]
    gets = [local(second_in.at[r], low.at[r], come.at[r]) for r in range(panels)]
    gets += [local(first_in, one, come.at[panels]), local(bias_in, bias, come.at[panels + 1])]
    puts = [local(wide.at[r], second.at[r], go.at[r]) for r in range(panels)] + [local(one, first, go.at[panels])]
    for get in gets:
        get.start()
    for r in range(panels):
        gets[r].wait()
        wide[r] = low[r].astype(F32)
        puts[r].start()
    gets[panels].wait()
    puts[panels].start()
    gets[panels + 1].wait()
    bias_one[...] = bias[:1]
    bias_two[...] = bias[1:2]
    for put in puts:
        put.wait()


def on_device(dims, features, adjacency_one, pre_hidden, adjacency_two, weight_two, out_grad):
    Y, X, Z, G, C = dims
    NP, ZZ = Y * X, Z * G
    blocks, cw, nb = features.shape[1:]
    relations, word_rows = adjacency_one.shape[2:4]
    dst, h = pre_hidden.shape[2:]
    seeds = out_grad.shape[2]
    half = (relations + 1) // C
    hc = h // NP
    factor = float(seeds * NP * ZZ * C) ** (-0.5)
    vmem = pltpu.VMEM
    any_spec = pl.BlockSpec(memory_space=pl.ANY)
    dma = pltpu.SemaphoreType.DMA
    shapes = dict(
        pre=vmem((dst, h), BF16),
        words2=vmem(adjacency_two.shape[2:], jnp.int32),
        w2=vmem(weight_two.shape, BF16),
        og=vmem((seeds, h), BF16),
        xv=vmem((blocks, cw, nb), BF16),
        words1=vmem((Z * relations, word_rows, nb), jnp.int32),
        dense2=vmem((relations, seeds, dst), BF16),
        dense1=vmem((Z * relations, dst, nb), BF16),
        rx=vmem((Z, TOP + NP * cw, nb), BF16),
        hgown=vmem((dst, h), BF16),
        hgbuf=vmem((Z, dst, h), BF16),
        gathered=vmem((relations, NP * cw, dst), BF16),
        total=vmem((dst, h), F32),
        weight2=vmem((relations, seeds, dst), F32),
        acc=vmem((relations + 1, NP * cw, h), F32),
        wg=vmem((relations + 1, h, h), F32),
        cxs2=vmem((half * h, h), BF16),
        cxr2=vmem((half * h, h), BF16),
        cxs1=vmem((half, NP * cw, h), BF16),
        cxr1=vmem((half, NP * cw, h), BF16),
        s1=vmem((NP, half * cw, h), BF16),
        r1=vmem((NP, half * cw, h), BF16),
        zhs=vmem((half, cw, h), BF16),
        zhr=vmem((half, cw, h), BF16),
        d1s=vmem((half, cw, h), F32),
        bias=vmem((8, h), F32),
        bs=vmem((1, h), F32),
        br=vmem((1, h), F32),
        bmine=vmem((1, h), F32),
        btheirs=vmem((1, h), F32),
        bplane=vmem((NP, 1, h), F32),
        bcol=vmem((ZZ, 1, h), F32),
        loc=dma((5 + Z,)),
        own=dma((Z,)),
        xs=dma((Z,)),
        xr=dma((Z,)),
        hs=dma((Z,)),
        hr=dma((Z,)),
        ss=dma((PHASES * half * PARTS,)),
        rs=dma((PHASES * half * PARTS,)),
        st=dma((half * PARTS + 2,)),
    )
    for n in range(half * PARTS):
        for name in ("s2", "r2", "ag"):
            shapes[f"{name}_{n}"] = vmem((NP, hc // PARTS, h), BF16)
        shapes[f"zb_{n}"] = vmem((ZZ, hc // PARTS, h), BF16)
    out1, out2, outb = pl.pallas_call(
        functools.partial(kernel, dims, factor, tuple(shapes)),
        name="graph_grads",
        out_shape=(
            jax.ShapeDtypeStruct((relations + 1, cw, h), F32),
            jax.ShapeDtypeStruct((relations + 1, NP, hc, h), BF16),
            jax.ShapeDtypeStruct((8, h), F32),
        ),
        in_specs=[any_spec] * 6,
        out_specs=(any_spec,) * 3,
        scratch_shapes=list(shapes.values()),
        compiler_params=pltpu.CompilerParams(
            collective_id=0, has_side_effects=True, vmem_limit_bytes=MAIN_LIMIT
        ),
    )(features, adjacency_one, pre_hidden, adjacency_two, weight_two, out_grad)
    panels = relations + 1
    vmem_spec = pl.BlockSpec(memory_space=pltpu.VMEM)
    first, second, bias_one, bias_two = pl.pallas_call(
        widen,
        name="widen",
        out_shape=(
            jax.ShapeDtypeStruct((panels, cw, h), F32),
            jax.ShapeDtypeStruct((panels, NP, hc, h), F32),
            jax.ShapeDtypeStruct((1, h), F32),
            jax.ShapeDtypeStruct((1, h), F32),
        ),
        in_specs=[any_spec] * 3,
        out_specs=(any_spec, any_spec, vmem_spec, vmem_spec),
        scratch_shapes=[
            vmem((panels, cw, h), F32),
            vmem((panels, NP, hc, h), BF16),
            vmem((panels, NP, hc, h), F32),
            vmem((8, h), F32),
            dma((panels + 2,)),
            dma((panels + 1,)),
        ],
        compiler_params=pltpu.CompilerParams(vmem_limit_bytes=WIDEN_LIMIT),
    )(out1, out2, outb)
    return first, bias_one.reshape(h), second.reshape(panels, h, h), bias_two.reshape(h)


def build(devices, dims):
    torus = Mesh(devices.reshape(dims), AXES)
    placed = (
        P(REP, None, FEAT, None),
        P(REP, None, None, None, None),
        P(REP, FEAT, None, None),
        P(REP, FEAT, None, None, None),
        P(),
        P(REP, FEAT, None, None),
    )
    return jax.shard_map(
        functools.partial(on_device, dims),
        mesh=torus,
        in_specs=placed,
        out_specs=(P(None, FEAT, None), P(), P(), P()),
        check_vma=False,
    )


def solution(mesh):
    dims = (4, 4, mesh.shape["feat"] // 16, mesh.shape["rep"] // 2, 2)
    return build(mesh.devices, dims)
```

```python
import functools
import types

import jax
import jax.numpy as jnp
from jax import lax
from jax.experimental import pallas as pl
from jax.experimental.pallas import tpu as pltpu
from jax.sharding import Mesh
from jax.sharding import PartitionSpec as P

MESH = pl.DeviceIdType.MESH
AXES = ("y", "x", "z", "g", "c")
FEAT = ("y", "x", "z")
REP = ("g", "c")
BF16 = jnp.bfloat16
F32 = jnp.float32
NN = (((1,), (0,)), ((), ()))
NT = (((1,), (1,)), ((), ()))
TN = (((0,), (0,)), ((), ()))
WIDEN_LIMIT = 16 * 2**20
MAIN_LIMIT = 48 * 2**20
TOP = 16
PAIR = 2
PHASES = 13
SWAP2, RS2, COL, AG, SWAP3, SWAP1, RS1, CROSS, SWAP4, BSWAP, BPLANE, BCOL, BLAST = range(PHASES)


def mm(a, b, dims):
    return lax.dot_general(a, b, dims, preferred_element_type=F32)


def local(src, dst, sem):
    return pltpu.make_async_copy(src, dst, sem)


def remote(src, dst, send, recv, device):
    return pltpu.make_async_remote_copy(
        src_ref=src, dst_ref=dst, send_sem=send, recv_sem=recv, device_id=device, device_id_type=MESH
    )


def spread_bits(words, r, out, rows, width):
    shift = lax.broadcasted_iota(jnp.int32, (16, width), 0)
    for w in range(rows // 16):
        word = jnp.broadcast_to(words[r, pl.ds(w, 1), :], (16, width))
        bits = lax.bitwise_and(lax.shift_right_logical(word, shift), 1)
        out[r, pl.ds(16 * w, 16), :] = bits.astype(F32).astype(BF16)


def spread_scaled(words, t, out, rows, width):
    mask = lax.shift_left(1, lax.broadcasted_iota(jnp.int32, (16, width), 0))
    for w in range(rows // 16):
        word = jnp.broadcast_to(words[t, pl.ds(w, 1), :], (16, width))
        out[t, pl.ds(16 * w, 16), :] = lax.bitwise_and(word, mask).astype(F32).astype(BF16)


def skip_loop(count, skipped, body):
    def step(t, carry):
        body(t)
        return carry

    lax.fori_loop(0, skipped, step, 0)
    if skipped + 1 < count:
        lax.fori_loop(skipped + 1, count, step, 0)


def kernel(dims, factor, names, feat, adj1, pre_any, adj2, w2_any, og_any, out1, out2, outb, *scratch):
    v = types.SimpleNamespace(**dict(zip(names, scratch)))
    Y, X, Z, G, C = dims
    NP, ZZ = Y * X, Z * G
    y, x, z, g, c = (lax.axis_index(a) for a in AXES)
    me = y * X + x
    zabs = g * Z + z
    relations = v.words1.shape[0] // Z
    panels = relations + 1
    count = panels // PAIR
    half = panels // C
    cw = feat.shape[2]
    seeds, h = v.og.shape
    dst = v.pre.shape[0]
    hc = h // NP
    base = me * Z
    partner = (y, x, z, g, 1 - c)
    across = (y, x, z, 1 - g, c)

    def send_sem(phase, q=0):
        return v.ss.at[phase * count + q]

    def recv_sem(phase, q=0):
        return v.rs.at[phase * count + q]

    rows_of = [lax.rem(y + d, Y) for d in range(Y)]
    cols_of = [lax.rem(x + d, X) for d in range(X)]
    pairs = [(dy, dx) for dy in range(Y) for dx in range(X) if dy or dx]
    pairs.sort(key=lambda p: -min(p[0], Y - p[0]) - min(p[1], X - p[1]))

    def over_plane(body, sign=1):
        for dy, dx in pairs:
            yy, xx = rows_of[(sign * dy) % Y], cols_of[(sign * dx) % X]
            body(dy * X + dx, yy * X + xx, (yy, xx, z, g, c))

    def over_column(body):
        def step(t):
            zz = lax.rem(zabs + ZZ // 2 + t, ZZ)
            body((y, x, lax.rem(zz, Z), lax.div(zz, Z), c))

        skip_loop(ZZ, ZZ - ZZ // 2, step)

    def minibatch(i):
        return lax.rem(z + i, 2) + 2 * lax.rem(lax.div(z, 2) + i // 2 if isinstance(i, int) else lax.div(z, 2) + lax.div(i, 2), 2)

    barrier = pltpu.get_barrier_semaphore()

    def greet(device):
        pl.semaphore_signal(barrier, inc=1, device_id=device, device_id_type=MESH)

    over_plane(lambda slot, other, device: greet(device))
    over_column(greet)
    greet(partner)

    loads = [
        local(adj2.at[0, 0], v.words2, v.loc.at[0]),
        local(pre_any.at[0, 0], v.pre, v.loc.at[1]),
        local(og_any.at[0, 0], v.og, v.loc.at[2]),
        local(w2_any, v.w2, v.loc.at[3]),
        local(feat.at[0], v.xv, v.loc.at[4]),
    ]
    for q in range(Z):
        loads.append(
            local(adj1.at[0, base + q], v.words1.at[pl.ds(q * relations, relations)], v.loc.at[5 + q])
        )
    for load in loads:
        load.start()
    v.rx[:, pl.ds(0, TOP), :] = jnp.ones((Z, TOP, v.rx.shape[2]), BF16)
    loads[0].wait()
    for r in range(relations):
        spread_bits(v.words2, r, v.dense2, seeds, h)

    for load in loads[1:4]:
        load.wait()
    scaled = v.og[...].astype(F32) * factor
    low = scaled.astype(BF16)
    ones = jnp.ones((h, h), BF16)
    v.total[...] = jnp.zeros_like(v.total)
    v.total[pl.ds(0, seeds), :] = mm(low, v.w2[0], NT)
    for r in range(relations):
        inverse = 1.0 / jnp.maximum(mm(v.dense2[r], ones, NN), 1.0)
        v.weight2[r] = inverse
        backed = (mm(low, v.w2[r + 1], NT) * inverse).astype(BF16)
        v.total[...] += mm(v.dense2[r], backed, TN)
    v.hgown[...] = jnp.where(v.pre[...] > 0, v.total[...], 0.0).astype(BF16)
    local(v.hgown, v.hgbuf.at[z], v.hr.at[0]).start()
    loads[4].wait()

    pl.semaphore_wait(barrier, NP + ZZ - 1)

    def give_grad(k):
        return remote(v.hgown, v.hgbuf.at[z], v.hs.at[k], v.hr.at[k], (y, x, minibatch(k), g, c))

    for k in range(1, Z):
        give_grad(k).start()

    def send_features(i, carry):
        m = minibatch(i)
        local(v.xv.at[base + m], v.rx.at[m, pl.ds(TOP, cw), :], v.own.at[i]).start()
        over_plane(
            lambda slot, other, device: remote(
                v.xv.at[other * Z + m],
                v.rx.at[m, pl.ds(TOP + slot * cw, cw), :],
                v.xs.at[i],
                v.xr.at[i],
                device,
            ).start()
        )
        return carry

    lax.fori_loop(0, Z, send_features, 0)

    hidden = jnp.maximum(v.pre[...], 0)
    scaled = v.og[...].astype(F32) * factor
    low = scaled.astype(BF16)
    v.wg[0] = mm(hidden[:seeds], low, TN)
    for r in range(relations):
        mixed = (mm(v.dense2[r], hidden, NN) * v.weight2[r]).astype(BF16)
        v.wg[r + 1] = mm(mixed, low, TN)
    v.bown[pl.ds(0, 1), :] = jnp.sum(v.hgown[...].astype(F32), axis=0, keepdims=True)
    v.bown[pl.ds(1, 1), :] = jnp.sum(scaled, axis=0, keepdims=True)

    def give_second():
        return remote(v.cxs2, v.cxr2, send_sem(SWAP2), recv_sem(SWAP2), partner)

    def give_bias():
        return remote(v.bown, v.btheirs, send_sem(BSWAP), recv_sem(BSWAP), partner)

    @pl.when(c == 0)
    def _():
        for q in range(panels):
            v.cxs2[q] = v.wg[q].astype(BF16)
        give_second().start()
        give_bias().start()

    for load in loads[5:]:
        load.wait()

    def spread_one(t, carry):
        spread_scaled(v.words1, t, v.dense1, 16 * v.words1.shape[1], v.words1.shape[2])
        return carry

    lax.fori_loop(0, Z * relations, spread_one, 0)

    s2 = [getattr(v, f"s2_{n}") for n in range(count)]
    r2 = [getattr(v, f"r2_{n}") for n in range(count)]
    zb = [getattr(v, f"zb_{n}") for n in range(count)]
    ag = [getattr(v, f"ag_{n}") for n in range(count)]

    @pl.when(c == 1)
    def _():
        give_bias().wait_recv()
        v.bplane[me] = v.bown[...] + v.btheirs[...]
        over_plane(
            lambda slot, other, device: remote(
                v.bplane.at[me], v.bplane.at[me], send_sem(BPLANE), recv_sem(BPLANE), device
            ).start()
        )
        give_second().wait_recv()
        for n in range(count):
            for p in range(PAIR):
                both = v.wg[PAIR * n + p] + v.cxr2[PAIR * n + p].astype(F32)
                s2[n][:, pl.ds(p * hc, hc), :] = both.astype(BF16).reshape(NP, hc, h)
            over_plane(
                lambda slot, other, device: remote(
                    s2[n].at[other], r2[n].at[slot], send_sem(RS2, n), recv_sem(RS2, n), device
                ).start()
            )

    v.acc[...] = jnp.zeros_like(v.acc)
    least = lax.shift_left(1, lax.rem(lax.broadcasted_iota(jnp.int32, (1, dst), 1), 16)).astype(F32)

    def one_minibatch(i, carry):
        m = minibatch(i)
        local(v.xv.at[base + m], v.rx.at[m, pl.ds(TOP, cw), :], v.own.at[i]).wait()
        arrived = v.rx.at[m, pl.ds(TOP + cw, (NP - 1) * cw), :]
        local(arrived, arrived, v.xr.at[i]).wait()
        local(v.hgown, v.hgbuf.at[m], v.hr.at[i]).wait()
        grad_m = v.hgbuf[m]
        v.acc[0] += mm(v.rx[m, pl.ds(TOP, NP * cw), pl.ds(0, dst)], grad_m, NN)
        for r in range(relations):
            product = mm(v.rx[m], v.dense1[m * relations + r], NT)
            weight = 1.0 / jnp.maximum(product[:1], least)
            v.gathered[r] = (product[TOP:] * weight).astype(BF16)
        for r in range(relations):
            v.acc[r + 1] += mm(v.gathered[r], grad_m, NN)
        return carry

    lax.fori_loop(0, Z, one_minibatch, 0)

    def give_first():
        return remote(v.cxs1, v.cxr1, send_sem(SWAP1), recv_sem(SWAP1), partner)

    def result_two(n, p):
        return remote(
            ag[n].at[:, pl.ds(p * hc, hc), :],
            out2.at[PAIR * n + p],
            v.ps.at[PAIR * n + p],
            v.pr.at[PAIR * n + p],
            partner,
        )

    def store_two(n, p):
        return local(ag[n].at[:, pl.ds(p * hc, hc), :], out2.at[PAIR * n + p], v.st.at[PAIR * n + p])

    def result_bias():
        return remote(v.bias, outb, send_sem(BLAST), recv_sem(BLAST), partner)

    def landed(ref, sem):
        local(ref, ref, sem).wait()

    for q in range(half):
        v.cxs1[q] = v.acc[(1 - c) * half + q].astype(BF16)
    give_first().start()
    give_first().wait_recv()
    for q in range(half):
        both = v.acc[c * half + q] + v.cxr1[q].astype(F32)
        v.s1[:, pl.ds(q * cw, cw), :] = both.astype(BF16).reshape(NP, cw, h)
    over_plane(
        lambda slot, other, device: remote(
            v.s1.at[slot], v.r1.at[slot], send_sem(RS1), recv_sem(RS1), device
        ).start(),
        -1,
    )

    @pl.when(c == 1)
    def _():
        for n in range(count):
            landed(r2[n].at[pl.ds(1, NP - 1)], recv_sem(RS2, n))
            summed = s2[n][me].astype(F32)
            for k in range(1, NP):
                summed += r2[n][k].astype(F32)
            zb[n][zabs] = summed.astype(BF16)
            over_column(
                lambda device: remote(
                    zb[n].at[zabs], zb[n].at[zabs], send_sem(COL, n), recv_sem(COL, n), device
                ).start()
            )
        landed(v.bplane.at[pl.ds(0, NP - 1)], recv_sem(BPLANE))
        v.bcol[zabs] = jnp.sum(v.bplane[...], axis=0)
        over_column(
            lambda device: remote(
                v.bcol.at[zabs], v.bcol.at[zabs], send_sem(BCOL), recv_sem(BCOL), device
            ).start()
        )
        for n in range(count):
            landed(zb[n].at[pl.ds(0, ZZ - 1)], recv_sem(COL, n))
            summed = zb[n][0].astype(F32)
            for k in range(1, ZZ):
                summed += zb[n][k].astype(F32)
            ag[n][me] = summed.astype(BF16)
            over_plane(
                lambda slot, other, device: remote(
                    ag[n].at[me], ag[n].at[me], send_sem(AG, n), recv_sem(AG, n), device
                ).start()
            )

    landed(v.r1.at[pl.ds(1, NP - 1)], recv_sem(RS1))
    summed = v.s1[0].astype(F32)
    for k in range(1, NP):
        summed += v.r1[k].astype(F32)
    v.zhs[...] = summed.astype(BF16).reshape(half, cw, h)
    cross = remote(v.zhs, v.zhr, send_sem(CROSS), recv_sem(CROSS), across)
    cross.start()

    @pl.when(c == 1)
    def _():
        landed(v.bcol.at[pl.ds(0, ZZ - 1)], recv_sem(BCOL))
        v.bias[...] = jnp.sum(v.bcol[...], axis=0)
        result_bias().start()
        local(v.bias, outb, v.st.at[panels]).start()
        for n in range(count):
            landed(ag[n].at[pl.ds(0, NP - 1)], recv_sem(AG, n))
            for p in range(PAIR):
                result_two(n, p).start()
                store_two(n, p).start()

    cross.wait_recv()
    v.d1s[...] = v.zhs[...].astype(F32) + v.zhr[...].astype(F32)
    result_one = remote(v.d1s, out1.at[pl.ds(c * half, half)], send_sem(SWAP4), recv_sem(SWAP4), partner)
    result_one.start()
    store_one = local(v.d1s, out1.at[pl.ds(c * half, half)], v.so)
    store_one.start()

    give_first().wait_send()
    landed(v.r1.at[pl.ds(1, NP - 1)], send_sem(RS1))
    cross.wait_send()

    @pl.when(c == 1)
    def _():
        landed(v.bplane.at[pl.ds(0, NP - 1)], send_sem(BPLANE))
        landed(v.bcol.at[pl.ds(0, ZZ - 1)], send_sem(BCOL))
        for n in range(count):
            landed(r2[n].at[pl.ds(1, NP - 1)], send_sem(RS2, n))
            landed(zb[n].at[pl.ds(0, ZZ - 1)], send_sem(COL, n))
            landed(ag[n].at[pl.ds(0, NP - 1)], send_sem(AG, n))
        result_bias().wait_send()
        local(v.bias, outb, v.st.at[panels]).wait()
        for q in range(panels):
            store_two(q // PAIR, q % PAIR).wait()
            result_two(q // PAIR, q % PAIR).wait_send()

    @pl.when(c == 0)
    def _():
        give_second().wait_send()
        give_bias().wait_send()
        result_bias().wait_recv()
        for q in range(panels):
            result_two(q // PAIR, q % PAIR).wait_recv()

    store_one.wait()
    result_one.wait()

    for i in range(Z):
        landed(v.xv.at[pl.ds(0, NP - 1)], v.xs.at[i])
    for k in range(1, Z):
        give_grad(k).wait_send()


def widen(first_in, second_in, bias_in, first, second, bias_one, bias_two, wide, go):
    panels = second_in.shape[0]
    puts = [local(wide.at[r], second.at[r], go.at[r]) for r in range(panels)]
    puts.append(local(first_in, first, go.at[panels]))
    puts[panels].start()
    for r in range(panels):
        wide[r] = second_in[r].astype(F32)
        puts[r].start()
    bias_one[...] = bias_in[:1]
    bias_two[...] = bias_in[1:2]
    for put in puts:
        put.wait()


def on_device(dims, features, adjacency_one, pre_hidden, adjacency_two, weight_two, out_grad):
    Y, X, Z, G, C = dims
    NP, ZZ = Y * X, Z * G
    blocks, cw, nb = features.shape[1:]
    relations, word_rows = adjacency_one.shape[2:4]
    dst, h = pre_hidden.shape[2:]
    seeds = out_grad.shape[2]
    hc = h // NP
    panels = relations + 1
    count = panels // PAIR
    half = panels // C
    factor = float(seeds * NP * ZZ * C) ** (-0.5)
    vmem = pltpu.VMEM
    any_spec = pl.BlockSpec(memory_space=pl.ANY)
    dma = pltpu.SemaphoreType.DMA
    shapes = dict(
        pre=vmem((dst, h), BF16),
        words2=vmem(adjacency_two.shape[2:], jnp.int32),
        w2=vmem(weight_two.shape, BF16),
        og=vmem((seeds, h), BF16),
        xv=vmem((blocks, cw, nb), BF16),
        words1=vmem((Z * relations, word_rows, nb), jnp.int32),
        dense2=vmem((relations, seeds, dst), BF16),
        dense1=vmem((Z * relations, dst, nb), BF16),
        rx=vmem((Z, TOP + NP * cw, nb), BF16),
        hgown=vmem((dst, h), BF16),
        hgbuf=vmem((Z, dst, h), BF16),
        gathered=vmem((relations, NP * cw, dst), BF16),
        total=vmem((dst, h), F32),
        weight2=vmem((relations, seeds, dst), F32),
        acc=vmem((relations + 1, NP * cw, h), F32),
        wg=vmem((relations + 1, h, h), F32),
        cxs2=vmem((panels, h, h), BF16),
        cxr2=vmem((panels, h, h), BF16),
        cxs1=vmem((half, NP * cw, h), BF16),
        cxr1=vmem((half, NP * cw, h), BF16),
        s1=vmem((NP, half * cw, h), BF16),
        r1=vmem((NP, half * cw, h), BF16),
        zhs=vmem((half, cw, h), BF16),
        zhr=vmem((half, cw, h), BF16),
        d1s=vmem((half, cw, h), F32),
        bias=vmem((2, h), F32),
        bown=vmem((2, h), F32),
        btheirs=vmem((2, h), F32),
        bplane=vmem((NP, 2, h), F32),
        bcol=vmem((ZZ, 2, h), F32),
        loc=dma((5 + Z,)),
        own=dma((Z,)),
        xs=dma((Z,)),
        xr=dma((Z,)),
        hs=dma((Z,)),
        hr=dma((Z,)),
        ss=dma((PHASES * count,)),
        rs=dma((PHASES * count,)),
        ps=dma((panels,)),
        pr=dma((panels,)),
        st=dma((panels + 1,)),
        so=pltpu.SemaphoreType.DMA,
    )
    for n in range(count):
        for name in ("s2", "r2", "ag"):
            shapes[f"{name}_{n}"] = vmem((NP, PAIR * hc, h), BF16)
        shapes[f"zb_{n}"] = vmem((ZZ, PAIR * hc, h), BF16)
    out1, out2, outb = pl.pallas_call(
        functools.partial(kernel, dims, factor, tuple(shapes)),
        name="graph_grads",
        out_shape=(
            jax.ShapeDtypeStruct((relations + 1, cw, h), F32),
            jax.ShapeDtypeStruct((relations + 1, NP, hc, h), BF16),
            jax.ShapeDtypeStruct((2, h), F32),
        ),
        in_specs=[any_spec] * 6,
        out_specs=(any_spec,) * 3,
        scratch_shapes=list(shapes.values()),
        compiler_params=pltpu.CompilerParams(
            collective_id=0, has_side_effects=True, vmem_limit_bytes=MAIN_LIMIT
        ),
    )(
        *(
            pltpu.with_memory_space_constraint(a, pltpu.HBM)
            for a in (features, adjacency_one, pre_hidden, adjacency_two, weight_two, out_grad)
        )
    )
    vmem_spec = pl.BlockSpec(memory_space=pltpu.VMEM)
    first, second, bias_one, bias_two = pl.pallas_call(
        widen,
        name="widen",
        out_shape=(
            jax.ShapeDtypeStruct((panels, cw, h), F32),
            jax.ShapeDtypeStruct((panels, NP, hc, h), F32),
            jax.ShapeDtypeStruct((1, h), F32),
            jax.ShapeDtypeStruct((1, h), F32),
        ),
        in_specs=[vmem_spec] * 3,
        out_specs=(any_spec, any_spec, vmem_spec, vmem_spec),
        scratch_shapes=[
            vmem((panels, NP, hc, h), F32),
            dma((panels + 1,)),
        ],
        compiler_params=pltpu.CompilerParams(vmem_limit_bytes=WIDEN_LIMIT),
    )(out1, out2, outb)
    return first, bias_one.reshape(h), second.reshape(panels, h, h), bias_two.reshape(h)


def build(devices, dims):
    torus = Mesh(devices.reshape(dims), AXES)
    placed = (
        P(REP, None, FEAT, None),
        P(REP, None, None, None, None),
        P(REP, FEAT, None, None),
        P(REP, FEAT, None, None, None),
        P(),
        P(REP, FEAT, None, None),
    )
    return jax.shard_map(
        functools.partial(on_device, dims),
        mesh=torus,
        in_specs=placed,
        out_specs=(P(None, FEAT, None), P(), P(), P()),
        check_vma=False,
    )


def solution(mesh):
    dims = (4, 4, mesh.shape["feat"] // 16, mesh.shape["rep"] // 2, 2)
    return build(mesh.devices, dims)
```

```python
import functools
import types

import jax
import jax.numpy as jnp
from jax import lax
from jax.experimental import pallas as pl
from jax.experimental.pallas import tpu as pltpu
from jax.sharding import Mesh
from jax.sharding import PartitionSpec as P

MESH = pl.DeviceIdType.MESH
AXES = ("y", "x", "z", "g", "c")
FEAT = ("y", "x", "z")
REP = ("g", "c")
BF16 = jnp.bfloat16
F32 = jnp.float32
NN = (((1,), (0,)), ((), ()))
NT = (((1,), (1,)), ((), ()))
TN = (((0,), (0,)), ((), ()))
WIDEN_LIMIT = 16 * 2**20
MAIN_LIMIT = 48 * 2**20
TOP = 16
PAIR = 2
PHASES = 13
SWAP2, RS2, COL, AG, SWAP3, SWAP1, RS1, CROSS, SWAP4, BSWAP, BPLANE, BCOL, BLAST = range(PHASES)


def mm(a, b, dims):
    return lax.dot_general(a, b, dims, preferred_element_type=F32)


def local(src, dst, sem):
    return pltpu.make_async_copy(src, dst, sem)


def remote(src, dst, send, recv, device):
    return pltpu.make_async_remote_copy(
        src_ref=src, dst_ref=dst, send_sem=send, recv_sem=recv, device_id=device, device_id_type=MESH
    )


def spread_bits(words, r, out, rows, width):
    shift = lax.broadcasted_iota(jnp.int32, (16, width), 0)
    for w in range(rows // 16):
        word = jnp.broadcast_to(words[r, pl.ds(w, 1), :], (16, width))
        bits = lax.bitwise_and(lax.shift_right_logical(word, shift), 1)
        out[r, pl.ds(16 * w, 16), :] = bits.astype(F32).astype(BF16)


def spread_scaled(words, t, out, rows, width):
    mask = lax.shift_left(1, lax.broadcasted_iota(jnp.int32, (16, width), 0))
    for w in range(rows // 16):
        word = jnp.broadcast_to(words[t, pl.ds(w, 1), :], (16, width))
        out[t, pl.ds(16 * w, 16), :] = lax.bitwise_and(word, mask).astype(F32).astype(BF16)


def skip_loop(count, skipped, body):
    def step(t, carry):
        body(t)
        return carry

    lax.fori_loop(0, skipped, step, 0)
    if skipped + 1 < count:
        lax.fori_loop(skipped + 1, count, step, 0)


def kernel(dims, factor, names, feat, adj1, pre_any, adj2, w2_any, og_any, out1, out2, outb, *scratch):
    v = types.SimpleNamespace(**dict(zip(names, scratch)))
    Y, X, Z, G, C = dims
    NP, ZZ = Y * X, Z * G
    y, x, z, g, c = (lax.axis_index(a) for a in AXES)
    me = y * X + x
    zabs = g * Z + z
    relations = v.words1.shape[0] // Z
    panels = relations + 1
    count = panels // PAIR
    half = panels // C
    cw = feat.shape[2]
    seeds, h = v.og.shape
    dst = v.pre.shape[0]
    hc = h // NP
    base = me * Z
    partner = (y, x, z, g, 1 - c)
    across = (y, x, z, 1 - g, c)

    def send_sem(phase, q=0):
        return v.ss.at[phase * count + q]

    def recv_sem(phase, q=0):
        return v.rs.at[phase * count + q]

    rows_of = [lax.rem(y + d, Y) for d in range(Y)]
    cols_of = [lax.rem(x + d, X) for d in range(X)]
    pairs = [(dy, dx) for dy in range(Y) for dx in range(X) if dy or dx]
    pairs.sort(key=lambda p: -min(p[0], Y - p[0]) - min(p[1], X - p[1]))

    def over_plane(body, sign=1):
        for dy, dx in pairs:
            yy, xx = rows_of[(sign * dy) % Y], cols_of[(sign * dx) % X]
            body(dy * X + dx, yy * X + xx, (yy, xx, z, g, c))

    def over_column(body):
        def step(t):
            zz = lax.rem(zabs + ZZ // 2 + t, ZZ)
            body((y, x, lax.rem(zz, Z), lax.div(zz, Z), c))

        skip_loop(ZZ, ZZ - ZZ // 2, step)

    def minibatch(i):
        return lax.rem(z + i, 2) + 2 * lax.rem(lax.div(z, 2) + i // 2 if isinstance(i, int) else lax.div(z, 2) + lax.div(i, 2), 2)

    barrier = pltpu.get_barrier_semaphore()

    def greet(device):
        pl.semaphore_signal(barrier, inc=1, device_id=device, device_id_type=MESH)

    over_plane(lambda slot, other, device: greet(device))
    over_column(greet)
    greet(partner)

    loads = [
        local(adj2.at[0, 0], v.words2, v.loc.at[0]),
        local(pre_any.at[0, 0], v.pre, v.loc.at[1]),
        local(og_any.at[0, 0], v.og, v.loc.at[2]),
        local(w2_any, v.w2, v.loc.at[3]),
        local(feat.at[0], v.xv, v.loc.at[4]),
    ]
    for q in range(Z):
        loads.append(
            local(adj1.at[0, base + q], v.words1.at[pl.ds(q * relations, relations)], v.loc.at[5 + q])
        )
    for load in loads:
        load.start()
    v.rx[:, pl.ds(0, TOP), :] = jnp.ones((Z, TOP, v.rx.shape[2]), BF16)
    loads[0].wait()
    for r in range(relations):
        spread_bits(v.words2, r, v.dense2, seeds, h)

    for load in loads[1:4]:
        load.wait()
    scaled = v.og[...].astype(F32) * factor
    low = scaled.astype(BF16)
    ones = jnp.ones((h, h), BF16)
    v.total[...] = jnp.zeros_like(v.total)
    v.total[pl.ds(0, seeds), :] = mm(low, v.w2[0], NT)
    for r in range(relations):
        inverse = 1.0 / jnp.maximum(mm(v.dense2[r], ones, NN), 1.0)
        v.weight2[r] = inverse
        backed = (mm(low, v.w2[r + 1], NT) * inverse).astype(BF16)
        v.total[...] += mm(v.dense2[r], backed, TN)
    v.hgown[...] = jnp.where(v.pre[...] > 0, v.total[...], 0.0).astype(BF16)
    local(v.hgown, v.hgbuf.at[z], v.hr.at[0]).start()
    loads[4].wait()

    pl.semaphore_wait(barrier, NP + ZZ - 1)

    def give_grad(k):
        return remote(v.hgown, v.hgbuf.at[z], v.hs.at[k], v.hr.at[k], (y, x, minibatch(k), g, c))

    for k in range(1, Z):
        give_grad(k).start()

    def send_features(i, carry):
        m = minibatch(i)
        local(v.xv.at[base + m], v.rx.at[m, pl.ds(TOP, cw), :], v.own.at[i]).start()
        over_plane(
            lambda slot, other, device: remote(
                v.xv.at[other * Z + m],
                v.rx.at[m, pl.ds(TOP + slot * cw, cw), :],
                v.xs.at[i],
                v.xr.at[i],
                device,
            ).start()
        )
        return carry

    lax.fori_loop(0, Z, send_features, 0)

    hidden = jnp.maximum(v.pre[...], 0)
    scaled = v.og[...].astype(F32) * factor
    low = scaled.astype(BF16)
    v.wg[0] = mm(hidden[:seeds], low, TN)
    for r in range(relations):
        mixed = (mm(v.dense2[r], hidden, NN) * v.weight2[r]).astype(BF16)
        v.wg[r + 1] = mm(mixed, low, TN)
    v.bown[pl.ds(0, 1), :] = jnp.sum(v.hgown[...].astype(F32), axis=0, keepdims=True)
    v.bown[pl.ds(1, 1), :] = jnp.sum(scaled, axis=0, keepdims=True)

    def give_second():
        return remote(v.cxs2, v.cxr2, send_sem(SWAP2), recv_sem(SWAP2), partner)

    def give_bias():
        return remote(v.bown, v.btheirs, send_sem(BSWAP), recv_sem(BSWAP), partner)

    @pl.when(c == 0)
    def _():
        for q in range(panels):
            v.cxs2[q] = v.wg[q].astype(BF16)
        give_second().start()
        give_bias().start()

    for load in loads[5:]:
        load.wait()

    def spread_one(t, carry):
        spread_scaled(v.words1, t, v.dense1, 16 * v.words1.shape[1], v.words1.shape[2])
        return carry

    lax.fori_loop(0, Z * relations, spread_one, 0)

    s2 = [getattr(v, f"s2_{n}") for n in range(count)]
    r2 = [getattr(v, f"r2_{n}") for n in range(count)]
    zb = [getattr(v, f"zb_{n}") for n in range(count)]
    ag = [getattr(v, f"ag_{n}") for n in range(count)]

    @pl.when(c == 1)
    def _():
        give_bias().wait_recv()
        v.bplane[me] = v.bown[...] + v.btheirs[...]
        over_plane(
            lambda slot, other, device: remote(
                v.bplane.at[me], v.bplane.at[me], send_sem(BPLANE), recv_sem(BPLANE), device
            ).start()
        )
        give_second().wait_recv()
        for n in range(count):
            for p in range(PAIR):
                both = v.wg[PAIR * n + p] + v.cxr2[PAIR * n + p].astype(F32)
                s2[n][:, pl.ds(p * hc, hc), :] = both.astype(BF16).reshape(NP, hc, h)
            over_plane(
                lambda slot, other, device: remote(
                    s2[n].at[other], r2[n].at[slot], send_sem(RS2, n), recv_sem(RS2, n), device
                ).start()
            )

    v.acc[...] = jnp.zeros_like(v.acc)
    least = lax.shift_left(1, lax.rem(lax.broadcasted_iota(jnp.int32, (1, dst), 1), 16)).astype(F32)

    def one_minibatch(i, carry):
        m = minibatch(i)
        local(v.xv.at[base + m], v.rx.at[m, pl.ds(TOP, cw), :], v.own.at[i]).wait()
        arrived = v.rx.at[m, pl.ds(TOP + cw, (NP - 1) * cw), :]
        local(arrived, arrived, v.xr.at[i]).wait()
        local(v.hgown, v.hgbuf.at[m], v.hr.at[i]).wait()
        grad_m = v.hgbuf[m]
        v.acc[0] += mm(v.rx[m, pl.ds(TOP, NP * cw), pl.ds(0, dst)], grad_m, NN)
        for r in range(relations):
            product = mm(v.rx[m], v.dense1[m * relations + r], NT)
            weight = 1.0 / jnp.maximum(product[:1], least)
            v.gathered[r] = (product[TOP:] * weight).astype(BF16)
        for r in range(relations):
            v.acc[r + 1] += mm(v.gathered[r], grad_m, NN)
        return carry

    lax.fori_loop(0, Z, one_minibatch, 0)

    def give_first():
        return remote(v.cxs1, v.cxr1, send_sem(SWAP1), recv_sem(SWAP1), partner)

    def result_two(n, p):
        return remote(
            ag[n].at[:, pl.ds(p * hc, hc), :],
            out2.at[PAIR * n + p],
            v.ps.at[PAIR * n + p],
            v.pr.at[PAIR * n + p],
            partner,
        )

    def store_two(n, p):
        return local(ag[n].at[:, pl.ds(p * hc, hc), :], out2.at[PAIR * n + p], v.st.at[PAIR * n + p])

    def result_bias():
        return remote(v.bias, outb, send_sem(BLAST), recv_sem(BLAST), partner)

    def landed(ref, sem):
        local(ref, ref, sem).wait()

    for q in range(half):
        v.cxs1[q] = v.acc[(1 - c) * half + q].astype(BF16)
    give_first().start()

    @pl.when(c == 1)
    def _():
        for n in range(count):
            landed(r2[n].at[pl.ds(1, NP - 1)], recv_sem(RS2, n))
            summed = s2[n][me].astype(F32)
            for k in range(1, NP):
                summed += r2[n][k].astype(F32)
            zb[n][zabs] = summed.astype(BF16)
            over_column(
                lambda device: remote(
                    zb[n].at[zabs], zb[n].at[zabs], send_sem(COL, n), recv_sem(COL, n), device
                ).start()
            )
        landed(v.bplane.at[pl.ds(0, NP - 1)], recv_sem(BPLANE))
        v.bcol[zabs] = jnp.sum(v.bplane[...], axis=0)
        over_column(
            lambda device: remote(
                v.bcol.at[zabs], v.bcol.at[zabs], send_sem(BCOL), recv_sem(BCOL), device
            ).start()
        )

    give_first().wait_recv()
    for q in range(half):
        both = v.acc[c * half + q] + v.cxr1[q].astype(F32)
        v.s1[:, pl.ds(q * cw, cw), :] = both.astype(BF16).reshape(NP, cw, h)
    over_plane(
        lambda slot, other, device: remote(
            v.s1.at[slot], v.r1.at[slot], send_sem(RS1), recv_sem(RS1), device
        ).start(),
        -1,
    )

    @pl.when(c == 1)
    def _():
        for n in range(count):
            landed(zb[n].at[pl.ds(0, ZZ - 1)], recv_sem(COL, n))
            summed = zb[n][0].astype(F32)
            for k in range(1, ZZ):
                summed += zb[n][k].astype(F32)
            ag[n][me] = summed.astype(BF16)
            over_plane(
                lambda slot, other, device: remote(
                    ag[n].at[me], ag[n].at[me], send_sem(AG, n), recv_sem(AG, n), device
                ).start()
            )

    landed(v.r1.at[pl.ds(1, NP - 1)], recv_sem(RS1))
    summed = v.s1[0].astype(F32)
    for k in range(1, NP):
        summed += v.r1[k].astype(F32)
    v.zhs[...] = summed.astype(BF16).reshape(half, cw, h)
    cross = remote(v.zhs, v.zhr, send_sem(CROSS), recv_sem(CROSS), across)
    cross.start()

    @pl.when(c == 1)
    def _():
        landed(v.bcol.at[pl.ds(0, ZZ - 1)], recv_sem(BCOL))
        v.bias[...] = jnp.sum(v.bcol[...], axis=0)
        result_bias().start()
        local(v.bias, outb, v.st.at[panels]).start()
        for n in range(count):
            landed(ag[n].at[pl.ds(0, NP - 1)], recv_sem(AG, n))
            for p in range(PAIR):
                result_two(n, p).start()
                store_two(n, p).start()

    cross.wait_recv()
    v.d1s[...] = v.zhs[...].astype(F32) + v.zhr[...].astype(F32)
    result_one = remote(v.d1s, out1.at[pl.ds(c * half, half)], send_sem(SWAP4), recv_sem(SWAP4), partner)
    result_one.start()
    store_one = local(v.d1s, out1.at[pl.ds(c * half, half)], v.so)
    store_one.start()

    give_first().wait_send()
    landed(v.r1.at[pl.ds(1, NP - 1)], send_sem(RS1))
    cross.wait_send()

    @pl.when(c == 1)
    def _():
        landed(v.bplane.at[pl.ds(0, NP - 1)], send_sem(BPLANE))
        landed(v.bcol.at[pl.ds(0, ZZ - 1)], send_sem(BCOL))
        for n in range(count):
            landed(r2[n].at[pl.ds(1, NP - 1)], send_sem(RS2, n))
            landed(zb[n].at[pl.ds(0, ZZ - 1)], send_sem(COL, n))
            landed(ag[n].at[pl.ds(0, NP - 1)], send_sem(AG, n))
        result_bias().wait_send()
        local(v.bias, outb, v.st.at[panels]).wait()
        for q in range(panels):
            store_two(q // PAIR, q % PAIR).wait()
            result_two(q // PAIR, q % PAIR).wait_send()

    @pl.when(c == 0)
    def _():
        give_second().wait_send()
        give_bias().wait_send()
        result_bias().wait_recv()
        for q in range(panels):
            result_two(q // PAIR, q % PAIR).wait_recv()

    store_one.wait()
    result_one.wait()

    for i in range(Z):
        landed(v.xv.at[pl.ds(0, NP - 1)], v.xs.at[i])
    for k in range(1, Z):
        give_grad(k).wait_send()


def widen(first_in, second_in, bias_in, first, second, bias_one, bias_two, wide, go):
    panels = second_in.shape[0]
    puts = [local(wide.at[r], second.at[r], go.at[r]) for r in range(panels)]
    puts.append(local(first_in, first, go.at[panels]))
    puts[panels].start()
    for r in range(panels):
        wide[r] = second_in[r].astype(F32)
        puts[r].start()
    bias_one[...] = bias_in[:1]
    bias_two[...] = bias_in[1:2]
    for put in puts:
        put.wait()


def on_device(dims, features, adjacency_one, pre_hidden, adjacency_two, weight_two, out_grad):
    Y, X, Z, G, C = dims
    NP, ZZ = Y * X, Z * G
    blocks, cw, nb = features.shape[1:]
    relations, word_rows = adjacency_one.shape[2:4]
    dst, h = pre_hidden.shape[2:]
    seeds = out_grad.shape[2]
    hc = h // NP
    panels = relations + 1
    count = panels // PAIR
    half = panels // C
    factor = float(seeds * NP * ZZ * C) ** (-0.5)
    vmem = pltpu.VMEM
    any_spec = pl.BlockSpec(memory_space=pl.ANY)
    dma = pltpu.SemaphoreType.DMA
    shapes = dict(
        pre=vmem((dst, h), BF16),
        words2=vmem(adjacency_two.shape[2:], jnp.int32),
        w2=vmem(weight_two.shape, BF16),
        og=vmem((seeds, h), BF16),
        xv=vmem((blocks, cw, nb), BF16),
        words1=vmem((Z * relations, word_rows, nb), jnp.int32),
        dense2=vmem((relations, seeds, dst), BF16),
        dense1=vmem((Z * relations, dst, nb), BF16),
        rx=vmem((Z, TOP + NP * cw, nb), BF16),
        hgown=vmem((dst, h), BF16),
        hgbuf=vmem((Z, dst, h), BF16),
        gathered=vmem((relations, NP * cw, dst), BF16),
        total=vmem((dst, h), F32),
        weight2=vmem((relations, seeds, dst), F32),
        acc=vmem((relations + 1, NP * cw, h), F32),
        wg=vmem((relations + 1, h, h), F32),
        cxs2=vmem((panels, h, h), BF16),
        cxr2=vmem((panels, h, h), BF16),
        cxs1=vmem((half, NP * cw, h), BF16),
        cxr1=vmem((half, NP * cw, h), BF16),
        s1=vmem((NP, half * cw, h), BF16),
        r1=vmem((NP, half * cw, h), BF16),
        zhs=vmem((half, cw, h), BF16),
        zhr=vmem((half, cw, h), BF16),
        d1s=vmem((half, cw, h), F32),
        bias=vmem((2, h), F32),
        bown=vmem((2, h), F32),
        btheirs=vmem((2, h), F32),
        bplane=vmem((NP, 2, h), F32),
        bcol=vmem((ZZ, 2, h), F32),
        loc=dma((5 + Z,)),
        own=dma((Z,)),
        xs=dma((Z,)),
        xr=dma((Z,)),
        hs=dma((Z,)),
        hr=dma((Z,)),
        ss=dma((PHASES * count,)),
        rs=dma((PHASES * count,)),
        ps=dma((panels,)),
        pr=dma((panels,)),
        st=dma((panels + 1,)),
        so=pltpu.SemaphoreType.DMA,
    )
    for n in range(count):
        for name in ("s2", "r2", "ag"):
            shapes[f"{name}_{n}"] = vmem((NP, PAIR * hc, h), BF16)
        shapes[f"zb_{n}"] = vmem((ZZ, PAIR * hc, h), BF16)
    out1, out2, outb = pl.pallas_call(
        functools.partial(kernel, dims, factor, tuple(shapes)),
        name="graph_grads",
        out_shape=(
            jax.ShapeDtypeStruct((relations + 1, cw, h), F32),
            jax.ShapeDtypeStruct((relations + 1, NP, hc, h), BF16),
            jax.ShapeDtypeStruct((2, h), F32),
        ),
        in_specs=[any_spec] * 6,
        out_specs=(any_spec,) * 3,
        scratch_shapes=list(shapes.values()),
        compiler_params=pltpu.CompilerParams(
            collective_id=0, has_side_effects=True, vmem_limit_bytes=MAIN_LIMIT
        ),
    )(
        *(
            pltpu.with_memory_space_constraint(a, pltpu.HBM)
            for a in (features, adjacency_one, pre_hidden, adjacency_two, weight_two, out_grad)
        )
    )
    vmem_spec = pl.BlockSpec(memory_space=pltpu.VMEM)
    first, second, bias_one, bias_two = pl.pallas_call(
        widen,
        name="widen",
        out_shape=(
            jax.ShapeDtypeStruct((panels, cw, h), F32),
            jax.ShapeDtypeStruct((panels, NP, hc, h), F32),
            jax.ShapeDtypeStruct((1, h), F32),
            jax.ShapeDtypeStruct((1, h), F32),
        ),
        in_specs=[vmem_spec] * 3,
        out_specs=(any_spec, any_spec, vmem_spec, vmem_spec),
        scratch_shapes=[
            vmem((panels, NP, hc, h), F32),
            dma((panels + 1,)),
        ],
        compiler_params=pltpu.CompilerParams(vmem_limit_bytes=WIDEN_LIMIT),
    )(out1, out2, outb)
    return first, bias_one.reshape(h), second.reshape(panels, h, h), bias_two.reshape(h)


def build(devices, dims):
    torus = Mesh(devices.reshape(dims), AXES)
    placed = (
        P(REP, None, FEAT, None),
        P(REP, None, None, None, None),
        P(REP, FEAT, None, None),
        P(REP, FEAT, None, None, None),
        P(),
        P(REP, FEAT, None, None),
    )
    return jax.shard_map(
        functools.partial(on_device, dims),
        mesh=torus,
        in_specs=placed,
        out_specs=(P(None, FEAT, None), P(), P(), P()),
        check_vma=False,
    )


def solution(mesh):
    dims = (4, 4, mesh.shape["feat"] // 16, mesh.shape["rep"] // 2, 2)
    return build(mesh.devices, dims)
```

```python
import functools
import types

import jax
import jax.numpy as jnp
from jax import lax
from jax.experimental import pallas as pl
from jax.experimental.pallas import tpu as pltpu
from jax.sharding import Mesh
from jax.sharding import PartitionSpec as P

MESH = pl.DeviceIdType.MESH
AXES = ("y", "x", "z", "g", "c")
FEAT = ("y", "x", "z")
REP = ("g", "c")
BF16 = jnp.bfloat16
F32 = jnp.float32
NN = (((1,), (0,)), ((), ()))
NT = (((1,), (1,)), ((), ()))
TN = (((0,), (0,)), ((), ()))
WIDEN_LIMIT = 16 * 2**20
MAIN_LIMIT = 48 * 2**20
TOP = 16
PAIR = 2
CHUNKED = 3
SINGLE = 9
RS2, COL, AG = range(CHUNKED)
SWAP2, SWAP1, RS1, CROSS, SWAP4, BSWAP, BPLANE, BCOL, BLAST = range(CHUNKED, CHUNKED + SINGLE)


def mm(a, b, dims):
    return lax.dot_general(a, b, dims, preferred_element_type=F32)


def local(src, dst, sem):
    return pltpu.make_async_copy(src, dst, sem)


def remote(src, dst, send, recv, device):
    return pltpu.make_async_remote_copy(
        src_ref=src, dst_ref=dst, send_sem=send, recv_sem=recv, device_id=device, device_id_type=MESH
    )


def spread_bits(words, r, out, rows, width):
    shift = lax.broadcasted_iota(jnp.int32, (16, width), 0)
    for w in range(rows // 16):
        word = jnp.broadcast_to(words[r, pl.ds(w, 1), :], (16, width))
        bits = lax.bitwise_and(lax.shift_right_logical(word, shift), 1)
        out[r, pl.ds(16 * w, 16), :] = bits.astype(F32).astype(BF16)


def spread_scaled(words, t, out, rows, width):
    mask = lax.shift_left(1, lax.broadcasted_iota(jnp.int32, (16, width), 0))
    for w in range(rows // 16):
        word = jnp.broadcast_to(words[t, pl.ds(w, 1), :], (16, width))
        out[t, pl.ds(16 * w, 16), :] = lax.bitwise_and(word, mask).astype(F32).astype(BF16)


def skip_loop(count, skipped, body):
    def step(t, carry):
        body(t)
        return carry

    lax.fori_loop(0, skipped, step, 0)
    if skipped + 1 < count:
        lax.fori_loop(skipped + 1, count, step, 0)


def kernel(dims, factor, names, feat, adj1, pre_any, adj2, w2_any, og_any, out1, out2, outb, *scratch):
    v = types.SimpleNamespace(**dict(zip(names, scratch)))
    Y, X, Z, G, C = dims
    NP, ZZ = Y * X, Z * G
    y, x, z, g, c = (lax.axis_index(a) for a in AXES)
    me = y * X + x
    zabs = g * Z + z
    relations = v.words1.shape[0] // Z
    panels = relations + 1
    count = panels // PAIR
    half = panels // C
    cw = feat.shape[2]
    seeds, h = v.og.shape
    dst = v.pre.shape[0]
    hc = h // NP
    base = me * Z
    partner = (y, x, z, g, 1 - c)
    across = (y, x, z, 1 - g, c)

    def place(phase, n):
        return phase * count + n if phase < CHUNKED else CHUNKED * (count - 1) + phase

    def send_sem(phase, n=0):
        return v.ss.at[phase]

    def recv_sem(phase, n=0):
        return v.rs.at[place(phase, n)]

    rows_of = [lax.rem(y + d, Y) for d in range(Y)]
    cols_of = [lax.rem(x + d, X) for d in range(X)]
    pairs = [(dy, dx) for dy in range(Y) for dx in range(X) if dy or dx]
    pairs.sort(key=lambda p: -min(p[0], Y - p[0]) - min(p[1], X - p[1]))

    def over_plane(body, sign=1):
        for dy, dx in pairs:
            yy, xx = rows_of[(sign * dy) % Y], cols_of[(sign * dx) % X]
            body(dy * X + dx, yy * X + xx, (yy, xx, z, g, c))

    def over_column(body):
        def step(t):
            zz = lax.rem(zabs + ZZ // 2 + t, ZZ)
            body((y, x, lax.rem(zz, Z), lax.div(zz, Z), c))

        skip_loop(ZZ, ZZ - ZZ // 2, step)

    def minibatch(i):
        return lax.rem(z + i, 2) + 2 * lax.rem(lax.div(z, 2) + i // 2 if isinstance(i, int) else lax.div(z, 2) + lax.div(i, 2), 2)

    barrier = pltpu.get_barrier_semaphore()

    def greet(device):
        pl.semaphore_signal(barrier, inc=1, device_id=device, device_id_type=MESH)

    over_plane(lambda slot, other, device: greet(device))
    over_column(greet)
    greet(partner)

    loads = [
        local(adj2.at[0, 0], v.words2, v.loc.at[0]),
        local(pre_any.at[0, 0], v.pre, v.loc.at[1]),
        local(og_any.at[0, 0], v.og, v.loc.at[2]),
        local(w2_any, v.w2, v.loc.at[3]),
        local(feat.at[0], v.xv, v.loc.at[4]),
    ]
    for q in range(Z):
        loads.append(
            local(adj1.at[0, base + q], v.words1.at[pl.ds(q * relations, relations)], v.loc.at[5])
        )
    for load in loads:
        load.start()
    v.rx[:, pl.ds(0, TOP), :] = jnp.ones((Z, TOP, v.rx.shape[2]), BF16)
    loads[0].wait()
    for r in range(relations):
        spread_bits(v.words2, r, v.dense2, seeds, h)

    for load in loads[1:4]:
        load.wait()
    scaled = v.og[...].astype(F32) * factor
    low = scaled.astype(BF16)
    ones = jnp.ones((h, h), BF16)
    v.total[...] = jnp.zeros_like(v.total)
    v.total[pl.ds(0, seeds), :] = mm(low, v.w2[0], NT)
    for r in range(relations):
        inverse = 1.0 / jnp.maximum(mm(v.dense2[r], ones, NN), 1.0)
        v.weight2[r] = inverse
        backed = (mm(low, v.w2[r + 1], NT) * inverse).astype(BF16)
        v.total[...] += mm(v.dense2[r], backed, TN)
    v.hgown[...] = jnp.where(v.pre[...] > 0, v.total[...], 0.0).astype(BF16)
    local(v.hgown, v.hgbuf.at[z], v.hr.at[0]).start()
    loads[4].wait()

    pl.semaphore_wait(barrier, NP + ZZ - 1)

    def give_grad(k):
        return remote(v.hgown, v.hgbuf.at[z], v.hs.at[0], v.hr.at[k], (y, x, minibatch(k), g, c))

    for k in range(1, Z):
        give_grad(k).start()

    def send_features(i, carry):
        m = minibatch(i)
        local(v.xv.at[base + m], v.rx.at[m, pl.ds(TOP, cw), :], v.xr.at[i]).start()
        over_plane(
            lambda slot, other, device: remote(
                v.xv.at[other * Z + m],
                v.rx.at[m, pl.ds(TOP + slot * cw, cw), :],
                v.xs.at[0],
                v.xr.at[i],
                device,
            ).start()
        )
        return carry

    lax.fori_loop(0, Z, send_features, 0)

    hidden = jnp.maximum(v.pre[...], 0)
    scaled = v.og[...].astype(F32) * factor
    low = scaled.astype(BF16)
    v.wg[0] = mm(hidden[:seeds], low, TN)
    for r in range(relations):
        mixed = (mm(v.dense2[r], hidden, NN) * v.weight2[r]).astype(BF16)
        v.wg[r + 1] = mm(mixed, low, TN)
    v.bown[pl.ds(0, 1), :] = jnp.sum(v.hgown[...].astype(F32), axis=0, keepdims=True)
    v.bown[pl.ds(1, 1), :] = jnp.sum(scaled, axis=0, keepdims=True)

    def give_second():
        return remote(v.cxs2, v.cxr2, send_sem(SWAP2), recv_sem(SWAP2), partner)

    def give_bias():
        return remote(v.bown, v.btheirs, send_sem(BSWAP), recv_sem(BSWAP), partner)

    @pl.when(c == 0)
    def _():
        for q in range(panels):
            v.cxs2[q] = v.wg[q].astype(BF16)
        give_second().start()
        give_bias().start()

    local(v.words1, v.words1, v.loc.at[5]).wait()

    def spread_one(t, carry):
        spread_scaled(v.words1, t, v.dense1, 16 * v.words1.shape[1], v.words1.shape[2])
        return carry

    lax.fori_loop(0, Z * relations, spread_one, 0)

    s2, r2, zb, ag = ([ref.at[n] for n in range(count)] for ref in (v.s2, v.r2, v.zb, v.ag))

    @pl.when(c == 1)
    def _():
        give_bias().wait_recv()
        v.bplane[me] = v.bown[...] + v.btheirs[...]
        over_plane(
            lambda slot, other, device: remote(
                v.bplane.at[me], v.bplane.at[me], send_sem(BPLANE), recv_sem(BPLANE), device
            ).start()
        )
        give_second().wait_recv()
        for n in range(count):
            for p in range(PAIR):
                both = v.wg[PAIR * n + p] + v.cxr2[PAIR * n + p].astype(F32)
                s2[n][:, pl.ds(p * hc, hc), :] = both.astype(BF16).reshape(NP, hc, h)
            over_plane(
                lambda slot, other, device: remote(
                    s2[n].at[other], r2[n].at[slot], send_sem(RS2, n), recv_sem(RS2, n), device
                ).start()
            )

    v.acc[...] = jnp.zeros_like(v.acc)
    least = lax.shift_left(1, lax.rem(lax.broadcasted_iota(jnp.int32, (1, dst), 1), 16)).astype(F32)

    def one_minibatch(i, carry):
        m = minibatch(i)
        arrived = v.rx.at[m, pl.ds(TOP, NP * cw), :]
        local(arrived, arrived, v.xr.at[i]).wait()
        local(v.hgown, v.hgbuf.at[m], v.hr.at[i]).wait()
        grad_m = v.hgbuf[m]
        v.acc[0] += mm(v.rx[m, pl.ds(TOP, NP * cw), pl.ds(0, dst)], grad_m, NN)
        for r in range(relations):
            product = mm(v.rx[m], v.dense1[m * relations + r], NT)
            weight = 1.0 / jnp.maximum(product[:1], least)
            v.gathered[r] = (product[TOP:] * weight).astype(BF16)
        for r in range(relations):
            v.acc[r + 1] += mm(v.gathered[r], grad_m, NN)
        return carry

    lax.fori_loop(0, Z, one_minibatch, 0)

    def give_first():
        return remote(v.cxs1, v.cxr1, send_sem(SWAP1), recv_sem(SWAP1), partner)

    def result_two(n, p):
        return remote(
            ag[n].at[:, pl.ds(p * hc, hc), :],
            out2.at[PAIR * n + p],
            v.ps.at[0],
            v.ps.at[1],
            partner,
        )

    def store_two(n, p):
        return local(ag[n].at[:, pl.ds(p * hc, hc), :], out2.at[PAIR * n + p], v.st.at[0])

    def result_bias():
        return remote(v.bias, outb, send_sem(BLAST), recv_sem(BLAST), partner)

    def landed(ref, sem):
        local(ref, ref, sem).wait()

    for q in range(half):
        v.cxs1[q] = v.acc[(1 - c) * half + q].astype(BF16)
    give_first().start()

    @pl.when(c == 1)
    def _():
        for n in range(count):
            landed(r2[n].at[pl.ds(1, NP - 1)], recv_sem(RS2, n))
            summed = s2[n][me].astype(F32)
            for k in range(1, NP):
                summed += r2[n][k].astype(F32)
            zb[n][zabs] = summed.astype(BF16)
            over_column(
                lambda device: remote(
                    zb[n].at[zabs], zb[n].at[zabs], send_sem(COL, n), recv_sem(COL, n), device
                ).start()
            )
        landed(v.bplane.at[pl.ds(0, NP - 1)], recv_sem(BPLANE))
        v.bcol[zabs] = jnp.sum(v.bplane[...], axis=0)
        over_column(
            lambda device: remote(
                v.bcol.at[zabs], v.bcol.at[zabs], send_sem(BCOL), recv_sem(BCOL), device
            ).start()
        )

    give_first().wait_recv()
    for q in range(half):
        both = v.acc[c * half + q] + v.cxr1[q].astype(F32)
        v.s1[:, pl.ds(q * cw, cw), :] = both.astype(BF16).reshape(NP, cw, h)
    over_plane(
        lambda slot, other, device: remote(
            v.s1.at[slot], v.r1.at[slot], send_sem(RS1), recv_sem(RS1), device
        ).start(),
        -1,
    )

    @pl.when(c == 1)
    def _():
        for n in range(count):
            landed(zb[n].at[pl.ds(0, ZZ - 1)], recv_sem(COL, n))
            summed = zb[n][0].astype(F32)
            for k in range(1, ZZ):
                summed += zb[n][k].astype(F32)
            ag[n][me] = summed.astype(BF16)
            over_plane(
                lambda slot, other, device: remote(
                    ag[n].at[me], ag[n].at[me], send_sem(AG, n), recv_sem(AG, n), device
                ).start()
            )

    landed(v.r1.at[pl.ds(1, NP - 1)], recv_sem(RS1))
    summed = v.s1[0].astype(F32)
    for k in range(1, NP):
        summed += v.r1[k].astype(F32)
    v.zhs[...] = summed.astype(BF16).reshape(half, cw, h)
    cross = remote(v.zhs, v.zhr, send_sem(CROSS), recv_sem(CROSS), across)
    cross.start()

    @pl.when(c == 1)
    def _():
        landed(v.bcol.at[pl.ds(0, ZZ - 1)], recv_sem(BCOL))
        v.bias[...] = jnp.sum(v.bcol[...], axis=0)
        result_bias().start()
        local(v.bias, outb, v.st.at[1]).start()
        for n in range(count):
            landed(ag[n].at[pl.ds(0, NP - 1)], recv_sem(AG, n))
            for p in range(PAIR):
                result_two(n, p).start()
                store_two(n, p).start()

    cross.wait_recv()
    v.d1s[...] = v.zhs[...].astype(F32) + v.zhr[...].astype(F32)
    result_one = remote(v.d1s, out1.at[pl.ds(c * half, half)], send_sem(SWAP4), recv_sem(SWAP4), partner)
    result_one.start()
    store_one = local(v.d1s, out1.at[pl.ds(c * half, half)], v.so)
    store_one.start()

    give_first().wait_send()
    landed(v.r1.at[pl.ds(1, NP - 1)], send_sem(RS1))
    cross.wait_send()

    @pl.when(c == 1)
    def _():
        landed(v.bplane.at[pl.ds(0, NP - 1)], send_sem(BPLANE))
        landed(v.bcol.at[pl.ds(0, ZZ - 1)], send_sem(BCOL))
        landed(v.r2.at[:, pl.ds(1, NP - 1)], send_sem(RS2))
        landed(v.zb.at[:, pl.ds(0, ZZ - 1)], send_sem(COL))
        landed(v.ag.at[:, pl.ds(0, NP - 1)], send_sem(AG))
        result_bias().wait_send()
        local(v.bias, outb, v.st.at[1]).wait()
        landed(out2, v.st.at[0])
        landed(out2, v.ps.at[0])

    @pl.when(c == 0)
    def _():
        give_second().wait_send()
        give_bias().wait_send()
        result_bias().wait_recv()
        landed(out2, v.ps.at[1])

    store_one.wait()
    result_one.wait()

    landed(v.xv.at[pl.ds(0, Z * (NP - 1))], v.xs.at[0])
    landed(v.hgbuf.at[pl.ds(0, Z - 1)], v.hs.at[0])


def widen(first_in, second_in, bias_in, first, second, bias_one, bias_two, wide, go):
    panels = second_in.shape[0]
    puts = [local(wide.at[r], second.at[r], go.at[r]) for r in range(panels)]
    puts.append(local(first_in, first, go.at[panels]))
    puts.append(local(bias_in.at[pl.ds(0, 1)], bias_one, go.at[panels + 1]))
    puts.append(local(bias_in.at[pl.ds(1, 1)], bias_two, go.at[panels + 2]))
    for put in puts[panels:]:
        put.start()
    for r in range(panels):
        wide[r] = second_in[r].astype(F32)
        puts[r].start()
    for put in puts:
        put.wait()


def on_device(dims, features, adjacency_one, pre_hidden, adjacency_two, weight_two, out_grad):
    Y, X, Z, G, C = dims
    NP, ZZ = Y * X, Z * G
    blocks, cw, nb = features.shape[1:]
    relations, word_rows = adjacency_one.shape[2:4]
    dst, h = pre_hidden.shape[2:]
    seeds = out_grad.shape[2]
    hc = h // NP
    panels = relations + 1
    count = panels // PAIR
    half = panels // C
    factor = float(seeds * NP * ZZ * C) ** (-0.5)
    vmem = pltpu.VMEM
    any_spec = pl.BlockSpec(memory_space=pl.ANY)
    dma = pltpu.SemaphoreType.DMA
    shapes = dict(
        pre=vmem((dst, h), BF16),
        words2=vmem(adjacency_two.shape[2:], jnp.int32),
        w2=vmem(weight_two.shape, BF16),
        og=vmem((seeds, h), BF16),
        xv=vmem((blocks, cw, nb), BF16),
        words1=vmem((Z * relations, word_rows, nb), jnp.int32),
        dense2=vmem((relations, seeds, dst), BF16),
        dense1=vmem((Z * relations, dst, nb), BF16),
        rx=vmem((Z, TOP + NP * cw, nb), BF16),
        hgown=vmem((dst, h), BF16),
        hgbuf=vmem((Z, dst, h), BF16),
        gathered=vmem((relations, NP * cw, dst), BF16),
        total=vmem((dst, h), F32),
        weight2=vmem((relations, seeds, dst), F32),
        acc=vmem((relations + 1, NP * cw, h), F32),
        wg=vmem((relations + 1, h, h), F32),
        cxs2=vmem((panels, h, h), BF16),
        cxr2=vmem((panels, h, h), BF16),
        cxs1=vmem((half, NP * cw, h), BF16),
        cxr1=vmem((half, NP * cw, h), BF16),
        s1=vmem((NP, half * cw, h), BF16),
        r1=vmem((NP, half * cw, h), BF16),
        zhs=vmem((half, cw, h), BF16),
        zhr=vmem((half, cw, h), BF16),
        d1s=vmem((half, cw, h), F32),
        bias=vmem((2, h), F32),
        bown=vmem((2, h), F32),
        btheirs=vmem((2, h), F32),
        bplane=vmem((NP, 2, h), F32),
        bcol=vmem((ZZ, 2, h), F32),
        loc=dma((6,)),
        xs=dma((1,)),
        xr=dma((Z,)),
        hs=dma((1,)),
        hr=dma((Z,)),
        ss=dma((CHUNKED + SINGLE,)),
        rs=dma((CHUNKED * count + SINGLE,)),
        ps=dma((2,)),
        st=dma((2,)),
        so=pltpu.SemaphoreType.DMA,
    )
    for name in ("s2", "r2", "ag"):
        shapes[name] = vmem((count, NP, PAIR * hc, h), BF16)
    shapes["zb"] = vmem((count, ZZ, PAIR * hc, h), BF16)
    out1, out2, outb = pl.pallas_call(
        functools.partial(kernel, dims, factor, tuple(shapes)),
        name="graph_grads",
        out_shape=(
            jax.ShapeDtypeStruct((relations + 1, cw, h), F32),
            jax.ShapeDtypeStruct((relations + 1, NP, hc, h), BF16),
            jax.ShapeDtypeStruct((2, h), F32),
        ),
        in_specs=[any_spec] * 6,
        out_specs=(any_spec,) * 3,
        scratch_shapes=list(shapes.values()),
        compiler_params=pltpu.CompilerParams(
            collective_id=0, has_side_effects=True, vmem_limit_bytes=MAIN_LIMIT
        ),
    )(
        *(
            pltpu.with_memory_space_constraint(a, pltpu.HBM)
            for a in (features, adjacency_one, pre_hidden, adjacency_two, weight_two, out_grad)
        )
    )
    vmem_spec = pl.BlockSpec(memory_space=pltpu.VMEM)
    first, second, bias_one, bias_two = pl.pallas_call(
        widen,
        name="widen",
        out_shape=(
            jax.ShapeDtypeStruct((panels, cw, h), F32),
            jax.ShapeDtypeStruct((panels, NP, hc, h), F32),
            jax.ShapeDtypeStruct((1, h), F32),
            jax.ShapeDtypeStruct((1, h), F32),
        ),
        in_specs=[vmem_spec] * 3,
        out_specs=(any_spec,) * 4,
        scratch_shapes=[
            vmem((panels, NP, hc, h), F32),
            dma((panels + 3,)),
        ],
        compiler_params=pltpu.CompilerParams(vmem_limit_bytes=WIDEN_LIMIT),
    )(out1, out2, outb)
    return first, bias_one.reshape(h), second.reshape(panels, h, h), bias_two.reshape(h)


def build(devices, dims):
    torus = Mesh(devices.reshape(dims), AXES)
    placed = (
        P(REP, None, FEAT, None),
        P(REP, None, None, None, None),
        P(REP, FEAT, None, None),
        P(REP, FEAT, None, None, None),
        P(),
        P(REP, FEAT, None, None),
    )
    return jax.shard_map(
        functools.partial(on_device, dims),
        mesh=torus,
        in_specs=placed,
        out_specs=(P(None, FEAT, None), P(), P(), P()),
        check_vma=False,
    )


def solution(mesh):
    dims = (4, 4, mesh.shape["feat"] // 16, mesh.shape["rep"] // 2, 2)
    return build(mesh.devices, dims)
```

```python
import functools
import types

import jax
import jax.numpy as jnp
from jax import lax
from jax.experimental import pallas as pl
from jax.experimental.pallas import tpu as pltpu
from jax.sharding import Mesh
from jax.sharding import PartitionSpec as P

MESH = pl.DeviceIdType.MESH
AXES = ("y", "x", "z", "g", "c")
FEAT = ("y", "x", "z")
REP = ("g", "c")
BF16 = jnp.bfloat16
F32 = jnp.float32
NN = (((1,), (0,)), ((), ()))
NT = (((1,), (1,)), ((), ()))
TN = (((0,), (0,)), ((), ()))
WIDEN_LIMIT = 16 * 2**20
MAIN_LIMIT = 48 * 2**20
TOP = 16
PAIR = 2
CHUNKED = 3
SINGLE = 9
RS2, COL, AG = range(CHUNKED)
SWAP2, SWAP1, RS1, CROSS, SWAP4, BSWAP, BPLANE, BCOL, BLAST = range(CHUNKED, CHUNKED + SINGLE)


def mm(a, b, dims):
    return lax.dot_general(a, b, dims, preferred_element_type=F32)


def local(src, dst, sem):
    return pltpu.make_async_copy(src, dst, sem)


def remote(src, dst, send, recv, device):
    return pltpu.make_async_remote_copy(
        src_ref=src, dst_ref=dst, send_sem=send, recv_sem=recv, device_id=device, device_id_type=MESH
    )


def spread_bits(words, r, out, rows, width):
    shift = lax.broadcasted_iota(jnp.int32, (16, width), 0)
    for w in range(rows // 16):
        word = jnp.broadcast_to(words[r, pl.ds(w, 1), :], (16, width))
        bits = lax.bitwise_and(lax.shift_right_logical(word, shift), 1)
        out[r, pl.ds(16 * w, 16), :] = bits.astype(F32).astype(BF16)


def spread_scaled(words, t, out, rows, width):
    mask = lax.shift_left(1, lax.broadcasted_iota(jnp.int32, (16, width), 0))
    for w in range(rows // 16):
        word = jnp.broadcast_to(words[t, pl.ds(w, 1), :], (16, width))
        out[t, pl.ds(16 * w, 16), :] = lax.bitwise_and(word, mask).astype(F32).astype(BF16)


def skip_loop(count, skipped, body):
    def step(t, carry):
        body(t)
        return carry

    lax.fori_loop(0, skipped, step, 0)
    if skipped + 1 < count:
        lax.fori_loop(skipped + 1, count, step, 0)


def kernel(dims, factor, names, feat, adj1, pre_any, adj2, w2_any, og_any, out1, out2, outb, *scratch):
    v = types.SimpleNamespace(**dict(zip(names, scratch)))
    Y, X, Z, G, C = dims
    NP, ZZ = Y * X, Z * G
    y, x, z, g, c = (lax.axis_index(a) for a in AXES)
    me = y * X + x
    zabs = g * Z + z
    relations = v.words1.shape[0] // Z
    panels = relations + 1
    count = panels // PAIR
    half = panels // C
    cw = feat.shape[2]
    seeds, h = v.og.shape
    dst = v.pre.shape[0]
    hc = h // NP
    base = me * Z
    partner = (y, x, z, g, 1 - c)
    across = (y, x, z, 1 - g, c)

    def place(phase, n):
        return phase * count + n if phase < CHUNKED else CHUNKED * (count - 1) + phase

    def send_sem(phase, n=0):
        return v.ss.at[phase]

    def recv_sem(phase, n=0):
        return v.rs.at[place(phase, n)]

    rows_of = [lax.rem(y + d, Y) for d in range(Y)]
    cols_of = [lax.rem(x + d, X) for d in range(X)]
    pairs = [(dy, dx) for dy in range(Y) for dx in range(X) if dy or dx]
    pairs.sort(key=lambda p: -min(p[0], Y - p[0]) - min(p[1], X - p[1]))

    def over_plane(body, sign=1):
        for dy, dx in pairs:
            yy, xx = rows_of[(sign * dy) % Y], cols_of[(sign * dx) % X]
            body(dy * X + dx, yy * X + xx, (yy, xx, z, g, c))

    def over_column(body):
        def step(t):
            zz = lax.rem(zabs + ZZ // 2 + t, ZZ)
            body((y, x, lax.rem(zz, Z), lax.div(zz, Z), c))

        skip_loop(ZZ, ZZ - ZZ // 2, step)

    def minibatch(i):
        return lax.rem(z + i, 2) + 2 * lax.rem(lax.div(z, 2) + i // 2 if isinstance(i, int) else lax.div(z, 2) + lax.div(i, 2), 2)

    barrier = pltpu.get_barrier_semaphore()

    def greet(device):
        pl.semaphore_signal(barrier, inc=1, device_id=device, device_id_type=MESH)

    over_plane(lambda slot, other, device: greet(device))
    over_column(greet)
    greet(partner)

    loads = [
        local(adj2.at[0, 0], v.words2, v.loc.at[0]),
        local(pre_any.at[0, 0], v.pre, v.loc.at[1]),
        local(og_any.at[0, 0], v.og, v.loc.at[2]),
        local(w2_any, v.w2, v.loc.at[3]),
        local(feat.at[0], v.xv, v.loc.at[4]),
    ]
    for q in range(Z):
        loads.append(
            local(adj1.at[0, base + q], v.words1.at[pl.ds(q * relations, relations)], v.loc.at[5])
        )
    for load in loads:
        load.start()
    v.rx[:, pl.ds(0, TOP), :] = jnp.ones((Z, TOP, v.rx.shape[2]), BF16)
    loads[0].wait()
    for r in range(relations):
        spread_bits(v.words2, r, v.dense2, seeds, h)

    loads[4].wait()
    pl.semaphore_wait(barrier, NP + ZZ - 1)

    def send_features(i, carry):
        m = minibatch(i)
        local(v.xv.at[base + m], v.rx.at[m, pl.ds(TOP, cw), :], v.xr.at[i]).start()
        over_plane(
            lambda slot, other, device: remote(
                v.xv.at[other * Z + m],
                v.rx.at[m, pl.ds(TOP + slot * cw, cw), :],
                v.xs.at[0],
                v.xr.at[i],
                device,
            ).start()
        )
        return carry

    lax.fori_loop(0, Z, send_features, 0)

    for load in loads[1:4]:
        load.wait()
    scaled = v.og[...].astype(F32) * factor
    low = scaled.astype(BF16)
    ones = jnp.ones((h, h), BF16)
    v.total[...] = jnp.zeros_like(v.total)
    v.total[pl.ds(0, seeds), :] = mm(low, v.w2[0], NT)
    for r in range(relations):
        inverse = 1.0 / jnp.maximum(mm(v.dense2[r], ones, NN), 1.0)
        v.weight2[r] = inverse
        backed = (mm(low, v.w2[r + 1], NT) * inverse).astype(BF16)
        v.total[...] += mm(v.dense2[r], backed, TN)
    v.hgown[...] = jnp.where(v.pre[...] > 0, v.total[...], 0.0).astype(BF16)
    local(v.hgown, v.hgbuf.at[z], v.hr.at[0]).start()

    def give_grad(k):
        return remote(v.hgown, v.hgbuf.at[z], v.hs.at[0], v.hr.at[k], (y, x, minibatch(k), g, c))

    for k in range(1, Z):
        give_grad(k).start()

    hidden = jnp.maximum(v.pre[...], 0)
    scaled = v.og[...].astype(F32) * factor
    low = scaled.astype(BF16)
    v.wg[0] = mm(hidden[:seeds], low, TN)
    for r in range(relations):
        mixed = (mm(v.dense2[r], hidden, NN) * v.weight2[r]).astype(BF16)
        v.wg[r + 1] = mm(mixed, low, TN)
    v.bown[pl.ds(0, 1), :] = jnp.sum(v.hgown[...].astype(F32), axis=0, keepdims=True)
    v.bown[pl.ds(1, 1), :] = jnp.sum(scaled, axis=0, keepdims=True)

    def give_second():
        return remote(v.cxs2, v.cxr2, send_sem(SWAP2), recv_sem(SWAP2), partner)

    def give_bias():
        return remote(v.bown, v.btheirs, send_sem(BSWAP), recv_sem(BSWAP), partner)

    @pl.when(c == 0)
    def _():
        for q in range(panels):
            v.cxs2[q] = v.wg[q].astype(BF16)
        give_second().start()
        give_bias().start()

    local(v.words1, v.words1, v.loc.at[5]).wait()

    def spread_one(t, carry):
        spread_scaled(v.words1, t, v.dense1, 16 * v.words1.shape[1], v.words1.shape[2])
        return carry

    lax.fori_loop(0, Z * relations, spread_one, 0)

    s2, r2, zb, ag = ([ref.at[n] for n in range(count)] for ref in (v.s2, v.r2, v.zb, v.ag))

    @pl.when(c == 1)
    def _():
        give_bias().wait_recv()
        v.bplane[me] = v.bown[...] + v.btheirs[...]
        over_plane(
            lambda slot, other, device: remote(
                v.bplane.at[me], v.bplane.at[me], send_sem(BPLANE), recv_sem(BPLANE), device
            ).start()
        )
        give_second().wait_recv()
        for n in range(count):
            for p in range(PAIR):
                both = v.wg[PAIR * n + p] + v.cxr2[PAIR * n + p].astype(F32)
                s2[n][:, pl.ds(p * hc, hc), :] = both.astype(BF16).reshape(NP, hc, h)
            over_plane(
                lambda slot, other, device: remote(
                    s2[n].at[other], r2[n].at[slot], send_sem(RS2, n), recv_sem(RS2, n), device
                ).start()
            )

    v.acc[...] = jnp.zeros_like(v.acc)
    least = lax.shift_left(1, lax.rem(lax.broadcasted_iota(jnp.int32, (1, dst), 1), 16)).astype(F32)

    def one_minibatch(i, carry):
        m = minibatch(i)
        arrived = v.rx.at[m, pl.ds(TOP, NP * cw), :]
        local(arrived, arrived, v.xr.at[i]).wait()
        local(v.hgown, v.hgbuf.at[m], v.hr.at[i]).wait()
        grad_m = v.hgbuf[m]
        v.acc[0] += mm(v.rx[m, pl.ds(TOP, NP * cw), pl.ds(0, dst)], grad_m, NN)
        for r in range(relations):
            product = mm(v.rx[m], v.dense1[m * relations + r], NT)
            weight = 1.0 / jnp.maximum(product[:1], least)
            v.gathered[r] = (product[TOP:] * weight).astype(BF16)
        for r in range(relations):
            v.acc[r + 1] += mm(v.gathered[r], grad_m, NN)
        return carry

    lax.fori_loop(0, Z, one_minibatch, 0)

    def give_first():
        return remote(v.cxs1, v.cxr1, send_sem(SWAP1), recv_sem(SWAP1), partner)

    def result_two(n, p):
        return remote(
            ag[n].at[:, pl.ds(p * hc, hc), :],
            out2.at[PAIR * n + p],
            v.ps.at[0],
            v.ps.at[1],
            partner,
        )

    def store_two(n, p):
        return local(ag[n].at[:, pl.ds(p * hc, hc), :], out2.at[PAIR * n + p], v.st.at[0])

    def result_bias():
        return remote(v.bias, outb, send_sem(BLAST), recv_sem(BLAST), partner)

    def landed(ref, sem):
        local(ref, ref, sem).wait()

    for q in range(half):
        v.cxs1[q] = v.acc[(1 - c) * half + q].astype(BF16)
    give_first().start()

    @pl.when(c == 1)
    def _():
        for n in range(count):
            landed(r2[n].at[pl.ds(1, NP - 1)], recv_sem(RS2, n))
            summed = s2[n][me].astype(F32)
            for k in range(1, NP):
                summed += r2[n][k].astype(F32)
            zb[n][zabs] = summed.astype(BF16)
            over_column(
                lambda device: remote(
                    zb[n].at[zabs], zb[n].at[zabs], send_sem(COL, n), recv_sem(COL, n), device
                ).start()
            )
        landed(v.bplane.at[pl.ds(0, NP - 1)], recv_sem(BPLANE))
        v.bcol[zabs] = jnp.sum(v.bplane[...], axis=0)
        over_column(
            lambda device: remote(
                v.bcol.at[zabs], v.bcol.at[zabs], send_sem(BCOL), recv_sem(BCOL), device
            ).start()
        )

    give_first().wait_recv()
    for q in range(half):
        both = v.acc[c * half + q] + v.cxr1[q].astype(F32)
        v.s1[:, pl.ds(q * cw, cw), :] = both.astype(BF16).reshape(NP, cw, h)
    over_plane(
        lambda slot, other, device: remote(
            v.s1.at[slot], v.r1.at[slot], send_sem(RS1), recv_sem(RS1), device
        ).start(),
        -1,
    )

    @pl.when(c == 1)
    def _():
        for n in range(count):
            landed(zb[n].at[pl.ds(0, ZZ - 1)], recv_sem(COL, n))
            summed = zb[n][0].astype(F32)
            for k in range(1, ZZ):
                summed += zb[n][k].astype(F32)
            ag[n][me] = summed.astype(BF16)
            over_plane(
                lambda slot, other, device: remote(
                    ag[n].at[me], ag[n].at[me], send_sem(AG, n), recv_sem(AG, n), device
                ).start()
            )

    landed(v.r1.at[pl.ds(1, NP - 1)], recv_sem(RS1))
    summed = v.s1[0].astype(F32)
    for k in range(1, NP):
        summed += v.r1[k].astype(F32)
    v.zhs[...] = summed.astype(BF16).reshape(half, cw, h)
    cross = remote(v.zhs, v.zhr, send_sem(CROSS), recv_sem(CROSS), across)
    cross.start()

    @pl.when(c == 1)
    def _():
        landed(v.bcol.at[pl.ds(0, ZZ - 1)], recv_sem(BCOL))
        v.bias[...] = jnp.sum(v.bcol[...], axis=0)
        result_bias().start()
        local(v.bias, outb, v.st.at[1]).start()
        for n in range(count):
            landed(ag[n].at[pl.ds(0, NP - 1)], recv_sem(AG, n))
            for p in range(PAIR):
                result_two(n, p).start()
                store_two(n, p).start()

    cross.wait_recv()
    v.d1s[...] = v.zhs[...].astype(F32) + v.zhr[...].astype(F32)
    result_one = remote(v.d1s, out1.at[pl.ds(c * half, half)], send_sem(SWAP4), recv_sem(SWAP4), partner)
    result_one.start()
    store_one = local(v.d1s, out1.at[pl.ds(c * half, half)], v.so)
    store_one.start()

    give_first().wait_send()
    landed(v.r1.at[pl.ds(1, NP - 1)], send_sem(RS1))
    cross.wait_send()

    @pl.when(c == 1)
    def _():
        landed(v.bplane.at[pl.ds(0, NP - 1)], send_sem(BPLANE))
        landed(v.bcol.at[pl.ds(0, ZZ - 1)], send_sem(BCOL))
        landed(v.r2.at[:, pl.ds(1, NP - 1)], send_sem(RS2))
        landed(v.zb.at[:, pl.ds(0, ZZ - 1)], send_sem(COL))
        landed(v.ag.at[:, pl.ds(0, NP - 1)], send_sem(AG))
        result_bias().wait_send()
        local(v.bias, outb, v.st.at[1]).wait()
        landed(out2, v.st.at[0])
        landed(out2, v.ps.at[0])

    @pl.when(c == 0)
    def _():
        give_second().wait_send()
        give_bias().wait_send()
        result_bias().wait_recv()
        landed(out2, v.ps.at[1])

    store_one.wait()
    result_one.wait()

    landed(v.xv.at[pl.ds(0, Z * (NP - 1))], v.xs.at[0])
    landed(v.hgbuf.at[pl.ds(0, Z - 1)], v.hs.at[0])


def widen(first_in, second_in, bias_in, first, second, bias_one, bias_two, wide, go):
    panels = second_in.shape[0]
    puts = [local(wide.at[r], second.at[r], go.at[r]) for r in range(panels)]
    puts.append(local(first_in, first, go.at[panels]))
    puts.append(local(bias_in.at[pl.ds(0, 1)], bias_one, go.at[panels + 1]))
    puts.append(local(bias_in.at[pl.ds(1, 1)], bias_two, go.at[panels + 2]))
    for put in puts[panels:]:
        put.start()
    for r in range(panels):
        wide[r] = second_in[r].astype(F32)
        puts[r].start()
    for put in puts:
        put.wait()


def on_device(dims, features, adjacency_one, pre_hidden, adjacency_two, weight_two, out_grad):
    Y, X, Z, G, C = dims
    NP, ZZ = Y * X, Z * G
    blocks, cw, nb = features.shape[1:]
    relations, word_rows = adjacency_one.shape[2:4]
    dst, h = pre_hidden.shape[2:]
    seeds = out_grad.shape[2]
    hc = h // NP
    panels = relations + 1
    count = panels // PAIR
    half = panels // C
    factor = float(seeds * NP * ZZ * C) ** (-0.5)
    vmem = pltpu.VMEM
    any_spec = pl.BlockSpec(memory_space=pl.ANY)
    dma = pltpu.SemaphoreType.DMA
    shapes = dict(
        pre=vmem((dst, h), BF16),
        words2=vmem(adjacency_two.shape[2:], jnp.int32),
        w2=vmem(weight_two.shape, BF16),
        og=vmem((seeds, h), BF16),
        xv=vmem((blocks, cw, nb), BF16),
        words1=vmem((Z * relations, word_rows, nb), jnp.int32),
        dense2=vmem((relations, seeds, dst), BF16),
        dense1=vmem((Z * relations, dst, nb), BF16),
        rx=vmem((Z, TOP + NP * cw, nb), BF16),
        hgown=vmem((dst, h), BF16),
        hgbuf=vmem((Z, dst, h), BF16),
        gathered=vmem((relations, NP * cw, dst), BF16),
        total=vmem((dst, h), F32),
        weight2=vmem((relations, seeds, dst), F32),
        acc=vmem((relations + 1, NP * cw, h), F32),
        wg=vmem((relations + 1, h, h), F32),
        cxs2=vmem((panels, h, h), BF16),
        cxr2=vmem((panels, h, h), BF16),
        cxs1=vmem((half, NP * cw, h), BF16),
        cxr1=vmem((half, NP * cw, h), BF16),
        s1=vmem((NP, half * cw, h), BF16),
        r1=vmem((NP, half * cw, h), BF16),
        zhs=vmem((half, cw, h), BF16),
        zhr=vmem((half, cw, h), BF16),
        d1s=vmem((half, cw, h), F32),
        bias=vmem((2, h), F32),
        bown=vmem((2, h), F32),
        btheirs=vmem((2, h), F32),
        bplane=vmem((NP, 2, h), F32),
        bcol=vmem((ZZ, 2, h), F32),
        loc=dma((6,)),
        xs=dma((1,)),
        xr=dma((Z,)),
        hs=dma((1,)),
        hr=dma((Z,)),
        ss=dma((CHUNKED + SINGLE,)),
        rs=dma((CHUNKED * count + SINGLE,)),
        ps=dma((2,)),
        st=dma((2,)),
        so=pltpu.SemaphoreType.DMA,
    )
    for name in ("s2", "r2", "ag"):
        shapes[name] = vmem((count, NP, PAIR * hc, h), BF16)
    shapes["zb"] = vmem((count, ZZ, PAIR * hc, h), BF16)
    out1, out2, outb = pl.pallas_call(
        functools.partial(kernel, dims, factor, tuple(shapes)),
        name="graph_grads",
        out_shape=(
            jax.ShapeDtypeStruct((relations + 1, cw, h), F32),
            jax.ShapeDtypeStruct((relations + 1, NP, hc, h), BF16),
            jax.ShapeDtypeStruct((2, h), F32),
        ),
        in_specs=[any_spec] * 6,
        out_specs=(any_spec,) * 3,
        scratch_shapes=list(shapes.values()),
        compiler_params=pltpu.CompilerParams(
            collective_id=0, has_side_effects=True, vmem_limit_bytes=MAIN_LIMIT
        ),
    )(
        *(
            pltpu.with_memory_space_constraint(a, pltpu.HBM)
            for a in (features, adjacency_one, pre_hidden, adjacency_two, weight_two, out_grad)
        )
    )
    vmem_spec = pl.BlockSpec(memory_space=pltpu.VMEM)
    first, second, bias_one, bias_two = pl.pallas_call(
        widen,
        name="widen",
        out_shape=(
            jax.ShapeDtypeStruct((panels, cw, h), F32),
            jax.ShapeDtypeStruct((panels, NP, hc, h), F32),
            jax.ShapeDtypeStruct((1, h), F32),
            jax.ShapeDtypeStruct((1, h), F32),
        ),
        in_specs=[vmem_spec] * 3,
        out_specs=(any_spec,) * 4,
        scratch_shapes=[
            vmem((panels, NP, hc, h), F32),
            dma((panels + 3,)),
        ],
        compiler_params=pltpu.CompilerParams(vmem_limit_bytes=WIDEN_LIMIT),
    )(out1, out2, outb)
    return first, bias_one.reshape(h), second.reshape(panels, h, h), bias_two.reshape(h)


def build(devices, dims):
    torus = Mesh(devices.reshape(dims), AXES)
    placed = (
        P(REP, None, FEAT, None),
        P(REP, None, None, None, None),
        P(REP, FEAT, None, None),
        P(REP, FEAT, None, None, None),
        P(),
        P(REP, FEAT, None, None),
    )
    return jax.shard_map(
        functools.partial(on_device, dims),
        mesh=torus,
        in_specs=placed,
        out_specs=(P(None, FEAT, None), P(), P(), P()),
        check_vma=False,
    )


def solution(mesh):
    dims = (4, 4, mesh.shape["feat"] // 16, mesh.shape["rep"] // 2, 2)
    return build(mesh.devices, dims)
```
